32 devices in a mesh: col: 4 (over z), row: 8 (over y, x, core).
Axes of the slice: x: 2, y: 2, z: 4, core: 2. Of those that a mesh axis runs over, the one named last changes fastest.
Arguments:
- img_emb: bfloat16 [16384, 1024], P(('row', 'col'))
- txt_emb: bfloat16 [16384, 1024], P(('row', 'col'))
- log_scale: float32 [], replicated
Outputs:
- output 1: float32 [], replicated
- output 2: bfloat16 [16384, 1024], P(('row', 'col'))
- output 3: bfloat16 [16384, 1024], P(('row', 'col'))
- output 4: float32 [], replicated
All inputs are finite; a program needn't handle non-finite values.
Results may differ from the reference program's by a relative error of at most 0.001.
Values are sent between devices in bfloat16 or wider.
A program may use at most 1 GiB of HBM per device.

```python
import jax
import jax.numpy as jnp
from jax import lax

ROWS_DEV = 512
SHARDS = 32
EMBED_DIM = 1024
BATCH = ROWS_DEV * SHARDS


def unit_rows(values):
    return values / jnp.sqrt(jnp.sum(values * values, axis=-1, keepdims=True))


def setup_inputs(seed: int = 0) -> dict:
    keys = jax.random.split(jax.random.key(seed), 5)
    shared_dir = unit_rows(jax.random.normal(keys[0], (EMBED_DIM,), jnp.float32))
    spread = (1.0 / EMBED_DIM) ** 0.5
    pair_part = jax.random.normal(keys[1], (BATCH, EMBED_DIM), jnp.float32) * spread
    noise_img = jax.random.normal(keys[2], (BATCH, EMBED_DIM), jnp.float32) * spread
    noise_txt = jax.random.normal(keys[3], (BATCH, EMBED_DIM), jnp.float32) * spread
    img_emb = unit_rows(0.7 * shared_dir + 0.5 * pair_part + 0.5 * noise_img)
    txt_emb = unit_rows(0.7 * shared_dir + 0.5 * pair_part + 0.5 * noise_txt)
    log_scale = jnp.log(jax.random.uniform(keys[4], (), jnp.float32, 10.0, 30.0))
    return {"img_emb": img_emb.astype(jnp.bfloat16), "txt_emb": txt_emb.astype(jnp.bfloat16), "log_scale": log_scale}


def reference(img_emb, txt_emb, log_scale):
    logit_scale = jnp.exp(log_scale)
    img_blocks = img_emb.reshape(SHARDS, ROWS_DEV, EMBED_DIM)
    txt_blocks = txt_emb.reshape(SHARDS, ROWS_DEV, EMBED_DIM)
    block_ids = jnp.arange(SHARDS)
    positions = jnp.arange(BATCH)
    inv_count = 1.0 / (2 * BATCH)

    def row_lse_of(img_block):
        logits = logit_scale * jnp.dot(img_block, txt_emb.T, preferred_element_type=jnp.float32)
        return jax.nn.logsumexp(logits, axis=1)

    def col_lse_of(txt_block):
        logits_t = logit_scale * jnp.dot(txt_block, img_emb.T, preferred_element_type=jnp.float32)
        return jax.nn.logsumexp(logits_t, axis=1)

    row_lse = lax.map(row_lse_of, img_blocks).reshape(BATCH)
    col_lse = lax.map(col_lse_of, txt_blocks).reshape(BATCH)
    pos_logits = logit_scale * jnp.sum(img_emb.astype(jnp.float32) * txt_emb.astype(jnp.float32), axis=1)
    total_loss = (jnp.sum(row_lse - pos_logits) + jnp.sum(col_lse - pos_logits)) * inv_count

    def img_grad_of(block_args):
        block_id, img_block, row_lse_blk = block_args
        logits = logit_scale * jnp.dot(img_block, txt_emb.T, preferred_element_type=jnp.float32)
        diag_mask = (block_id * ROWS_DEV + jnp.arange(ROWS_DEV))[:, None] == positions[None, :]
        grad_tile = (jnp.exp(logits - row_lse_blk[:, None]) + jnp.exp(logits - col_lse[None, :]) - jnp.where(diag_mask, 2.0, 0.0)) * inv_count
        d_block = logit_scale * jnp.dot(grad_tile.astype(jnp.bfloat16), txt_emb, preferred_element_type=jnp.float32)
        return d_block.astype(jnp.bfloat16), jnp.sum(grad_tile * logits)

    def txt_grad_of(block_args):
        block_id, txt_block, col_lse_blk = block_args
        logits_t = logit_scale * jnp.dot(txt_block, img_emb.T, preferred_element_type=jnp.float32)
        diag_mask = (block_id * ROWS_DEV + jnp.arange(ROWS_DEV))[:, None] == positions[None, :]
        grad_t = (jnp.exp(logits_t - row_lse[None, :]) + jnp.exp(logits_t - col_lse_blk[:, None]) - jnp.where(diag_mask, 2.0, 0.0)) * inv_count
        d_block = logit_scale * jnp.dot(grad_t.astype(jnp.bfloat16), img_emb, preferred_element_type=jnp.float32)
        return d_block.astype(jnp.bfloat16)

    d_img, dt_parts = lax.map(img_grad_of, (block_ids, img_blocks, row_lse.reshape(SHARDS, ROWS_DEV)))
    d_txt = lax.map(txt_grad_of, (block_ids, txt_blocks, col_lse.reshape(SHARDS, ROWS_DEV)))
    return total_loss, d_img.reshape(BATCH, EMBED_DIM), d_txt.reshape(BATCH, EMBED_DIM), jnp.sum(dt_parts)
```

```python
import functools

import jax
import jax.numpy as jnp
from jax import lax
from jax.experimental import pallas as pl
from jax.experimental.pallas import tpu as pltpu
from jax.sharding import PartitionSpec as P

F32, BF16 = jnp.float32, jnp.bfloat16
MESH_ID = pl.DeviceIdType.MESH
NT = (((1,), (1,)), ((), ()))
TN = (((0,), (0,)), ((), ()))
LOG2E = 1.4426950408889634

ROWS, DIM, CH = 512, 1024, 128
NI, NTX = 4 * ROWS, 8 * ROWS
BLK, PIECE, HALF = 512, 256, 64
QS, TWO = range(4), range(2)
BATCH = 32 * ROWS
INV = 1.0 / (2 * BATCH)


def img_at(slot, k):
    if slot in (1, 2):
        return BLK + (k // 2) * BLK + (2 - slot) * PIECE + (k % 2) * CH
    return slot * BLK + k * CH


def txt_at(slot, k):
    odd = {1: 0, 5: 1, 3: 2, 7: 3}
    if slot in odd:
        return (4 + k) * BLK + odd[slot] * CH
    if slot in (2, 6):
        return 2 * BLK + (k // 2) * BLK + (slot // 4) * PIECE + (k % 2) * CH
    return slot // 4 * BLK + k * CH


def rows_of(start):
    return pl.ds(pl.multiple_of(start, CH), CH)


def at(i):
    return slice(i * CH, i * CH + CH)


def one(i):
    return slice(i, i + 1)


def kernel(
    t_ref, img_ref, txt_ref,
    loss_ref, dimg_ref, dtxt_ref, dt_ref, e_hbm,
    imgs, txts, est, rs, ra, cs, ca, bvec, erow, ecol, grow, gcol,
    xb, rzl, cb, rc, ry, rzh, oimg, otxt,
    rsend, rrecv, csend, crecv, red, redr,
    s_in, s_est, s_erow, s_ecol, s_out,
    ag, sib, row, colm, redm, x3, x2, zls, core, y3, y2, zhs,
):
    a = lax.axis_index("row")
    z = lax.axis_index("col")
    y, x, c = a // 4, (a // 2) % 2, a % 2
    zl, zh = z % 2, z // 2

    def dev(dx=0, dy=0, dc=0, dzl=0, dzh=0):
        yy = (1 - y) if dy else y
        xx = (1 - x) if dx else x
        cc = (1 - c) if dc else c
        l = (1 - zl) if dzl else zl
        h = (1 - zh) if dzh else zh
        return {"row": yy * 4 + xx * 2 + cc, "col": h * 2 + l}

    def row_peer(p):
        return dev(dx=p // 2, dzl=p % 2)

    def col_peer(p):
        return dev(dc=p // 4, dy=(p // 2) % 2, dzh=p % 2)

    ROW_PEERS, COL_PEERS = range(1, 4), range(1, 8)

    def remote(src, dst, sem, to):
        return pltpu.make_async_remote_copy(src_ref=src, dst_ref=dst, send_sem=sem[0], recv_sem=sem[1], device_id=to, device_id_type=MESH_ID)

    def sems(ref, *i):
        return ref.at[(0, *i)], ref.at[(1, *i)]

    in_i = pltpu.make_async_copy(img_ref, imgs.at[pl.ds(0, ROWS), :], s_in.at[0])
    in_t = pltpu.make_async_copy(txt_ref, txts.at[pl.ds(0, ROWS), :], s_in.at[1])
    in_i.start()
    in_t.start()
    barrier = pltpu.get_barrier_semaphore()
    for p in ROW_PEERS:
        pl.semaphore_signal(barrier, inc=1, device_id=row_peer(p), device_id_type=MESH_ID)
    for p in COL_PEERS:
        pl.semaphore_signal(barrier, inc=1, device_id=col_peer(p), device_id_type=MESH_ID)
    in_i.wait()
    in_t.wait()
    pl.semaphore_wait(barrier, 10)

    to_x, to_y, to_c, to_zl, to_zh = dev(dx=1), dev(dy=1), dev(dc=1), dev(dzl=1), dev(dzh=1)

    def gi(src, dst, n, to):
        return lambda k: remote(imgs.at[rows_of(img_at(src, k)), :], imgs.at[rows_of(img_at(dst, k)), :], sems(ag, n, k), to)

    def gt(src, dst, n, to):
        return lambda k: remote(txts.at[rows_of(txt_at(src, k)), :], txts.at[rows_of(txt_at(dst, k)), :], sems(ag, n, k), to)

    g_zl, g_x0, g_x1 = gi(0, 1, 0, to_zl), gi(0, 2, 1, to_x), gi(1, 3, 2, to_x)
    g_zh, g_y0, g_y1 = gt(0, 1, 3, to_zh), gt(0, 2, 4, to_y), gt(1, 3, 5, to_y)

    def g_c(s, k):
        return remote(txts.at[rows_of(txt_at(s, k)), :], txts.at[rows_of(txt_at(s + 4, k)), :], sems(sib, s, k), to_c)

    for k in QS:
        g_zl(k).start()
        g_x0(k).start()
        g_y0(k).start()
        g_c(0, k).start()
    for k in QS:
        g_zh(k).start()

    scale = jnp.exp(jnp.full((1, CH), t_ref[0], F32))
    scale_w = jnp.concatenate([scale] * (BLK // CH), axis=1) * LOG2E

    rs[...] = jnp.zeros_like(rs)
    ra[...] = jnp.zeros_like(ra)
    cs[...] = jnp.zeros_like(cs)
    ca[...] = jnp.zeros_like(ca)

    def est_copy(p, i0, j0):
        i0 = pl.multiple_of(i0, PIECE)
        return pltpu.make_async_copy(est.at[p], e_hbm.at[pl.ds(j0 // CH, BLK // CH), pl.ds(i0, PIECE), :], s_est.at[p])

    def block(i0, j0, rows, p0, used=True):
        i0 = pl.multiple_of(i0, PIECE)
        j0 = pl.multiple_of(j0, BLK)
        pieces = [(p0 + n, n * PIECE) for n in range(rows // PIECE)]
        for p, r in pieces:
            if used is True:
                est_copy(p, i0 + r, j0).wait()
            else:
                @pl.when(used)
                def _():
                    est_copy(p, i0 + r, j0).wait()
        acc = lax.dot_general(imgs[pl.ds(i0, rows), :], txts[pl.ds(j0, BLK), :], NT, preferred_element_type=F32)
        e = jnp.exp2(acc * scale_w)
        ea = e * acc
        parts = [e[:, at(q)] for q in range(BLK // CH)]
        prods = [ea[:, at(q)] for q in range(BLK // CH)]
        for p, r in pieces:
            for q, part in enumerate(parts):
                est[p, q] = part[r:r + PIECE]
        rs[pl.ds(i0, rows), :] += sum(parts[1:], parts[0])
        ra[pl.ds(i0, rows), :] += sum(prods[1:], prods[0])
        cs[:, pl.ds(j0, BLK)] += jnp.sum(e.reshape(rows // 8, 8, BLK), axis=0)
        ca[:, pl.ds(j0, BLK)] += jnp.sum(ea.reshape(rows // 8, 8, BLK), axis=0)
        for p, r in pieces:
            est_copy(p, i0 + r, j0).start()

    def take_texts(k):
        g_zh(k).wait_recv()
        g_y1(k).start()
        g_c(1, k).start()

    def take_last(k):
        g_y1(k).wait_recv()
        g_c(3, k).start()

    def near(s, _):
        @pl.when(s == 0)
        def _():
            for k in QS:
                g_c(0, k).wait_recv()

        @pl.when(s > 0)
        def _():
            for h in TWO:
                k = 2 * (s - 1) + h
                g_zl(k).wait_recv()
                g_x1(k).start()
                g_y0(k).wait_recv()
                g_c(2, k).start()
            for h in TWO:
                k = 2 * (s - 1) + h
                g_x0(k).wait_recv()
                g_c(2, k).wait_recv()

        def body(n, _):
            block(s * BLK, n * BLK, BLK, 0, s + n > 0)
            block(n * BLK, (s + 1) * BLK, BLK, 2, s + n > 0)
            return 0

        lax.fori_loop(0, s + 1, body, 0)
        return 0

    lax.fori_loop(0, 3, near, 0)

    def far(q, _):
        take_last(q)
        take_texts(q + 1)
        g_c(1, q).wait_recv()
        g_c(3, q).wait_recv()
        for m in range(3):
            block(m * BLK, (4 + q) * BLK, BLK, 2 * m, True if m < 2 else q > 0)

        @pl.when(q == 1)
        def _():
            take_texts(3)

        for h in TWO:
            g_x1(2 * q + h).wait_recv()
        for n in QS:
            block(3 * BLK + q * PIECE, n * BLK, PIECE, n)
        return 0

    take_texts(0)
    lax.fori_loop(0, 2, far, 0)
    take_last(2)
    for n in TWO:
        block(3 * BLK, (4 + n) * BLK, BLK, 2 * n)

    def last(q, _):
        @pl.when(q == 3)
        def _():
            take_last(q)

        g_c(1, q).wait_recv()
        g_c(3, q).wait_recv()
        for m in QS:
            block(m * BLK, (4 + q) * BLK, BLK, 2 * m, True if m < 3 else q > 2)
        return 0

    lax.fori_loop(2, 4, last, 0)
    diag = jnp.zeros((CH, 128), F32)
    for k in QS:
        prod = imgs[at(k), :].astype(F32) * txts[at(k), :].astype(F32)
        for q in range(DIM // CH):
            diag += prod[:, at(q)]
    diag = jnp.sum(diag, axis=0, keepdims=True)
    for p in range(8):
        est_copy(p, 0, 0).wait()

    def get_row(slot, k, buf):
        return pltpu.make_async_copy(e_hbm.at[:, rows_of(img_at(slot, k)), :], erow.at[buf], s_erow.at[buf])

    def get_col(slot, k, buf):
        return pltpu.make_async_copy(e_hbm.at[txt_at(slot, k) // CH], ecol.at[buf], s_ecol.at[buf])

    get_row(3, 0, 0).start()
    get_col(7, 0, 0).start()

    for j in range(NTX // CH):
        csend[one(j), :] = jnp.sum(cs[:, at(j)], axis=0, keepdims=True)
    ex_col = [remote(csend, crecv.at[p - 1], sems(colm, p - 1), col_peer(p)) for p in COL_PEERS]
    for copy in ex_col:
        copy.start()
    for i in range(NI // CH):
        rsend[one(i), :] = jnp.sum(rs[at(i), :].T, axis=0, keepdims=True)
    ex_row = [remote(rsend, rrecv.at[p - 1], sems(row, p - 1), row_peer(p)) for p in ROW_PEERS]
    for copy in ex_row:
        copy.start()
    for copy in ex_col:
        copy.wait_recv()

    loss_v = -2.0 * scale * diag
    dt_v = (-2.0 * INV) * scale * diag
    dt_cols = jnp.zeros((8, CH), F32)
    for slot in range(8):
        for k in QS:
            j = txt_at(slot, k) // CH
            tot = csend[one(j), :]
            for p in COL_PEERS:
                tot += crecv[p - 1, one(txt_at(slot ^ p, k) // CH), :]
            if slot == 0:
                loss_v += jnp.log(tot)
            fac = INV / tot
            bvec[:, at(j)] = fac
            dt_cols += fac * ca[:, at(j)]
    for copy in ex_row:
        copy.wait_recv()
    dt_rows = jnp.zeros((CH, CH), F32)
    for slot in QS:
        for k in QS:
            i = img_at(slot, k) // CH
            tot = rsend[one(i), :]
            for p in ROW_PEERS:
                tot += rrecv[p - 1, one(img_at(slot ^ p, k) // CH), :]
            if slot == 0:
                loss_v += jnp.log(tot)
            fac = jnp.broadcast_to(INV / tot, (CH, CH)).T
            rs[at(i), :] = fac
            dt_rows += fac * ra[at(i), :]
    dt_v += scale * (jnp.sum(dt_rows, axis=0, keepdims=True) + jnp.sum(dt_cols, axis=0, keepdims=True))
    red[0] = jnp.concatenate([loss_v, dt_v, jnp.zeros((6, CH), F32)], axis=0)

    red_to = [to_x, to_zl, to_y, to_zh, to_c]
    ex_red = [remote(red.at[i], redr.at[i], sems(redm, i), to) for i, to in enumerate(red_to)]

    def red_step(i):
        ex_red[i].wait()
        red[i + 1] = red[i] + redr[i]
        if i + 1 < len(ex_red):
            ex_red[i + 1].start()

    ex_red[0].start()

    ri = lax.broadcasted_iota(jnp.int32, (CH, CH), 0)
    ci = lax.broadcasted_iota(jnp.int32, (CH, CH), 1)
    eye2 = jnp.where(ri == ci, 2.0 * INV, 0.0).astype(F32)

    def img_chunk(slot, k, buf, after):
        get_row(slot, k, buf).wait()
        after()
        fac = rs[rows_of(img_at(slot, k)), :]
        for j in range(NTX // CH):
            grow[:, at(j)] = (erow[buf, j] * (fac + bvec[:, at(j)])).astype(BF16)
        if slot == 0:
            j0 = pl.multiple_of(k * CH, CH)
            g = erow[buf, k] * (fac + bvec[:, pl.ds(j0, CH)])
            grow[:, pl.ds(j0, CH)] = (g - eye2).astype(BF16)
        return jnp.dot(grow[...], txts[...], preferred_element_type=F32)

    def txt_chunk(slot, k, buf, after):
        get_col(slot, k, buf).wait()
        after()
        b = bvec[:, pl.ds(pl.multiple_of(txt_at(slot, k), CH), CH)]
        gcol[...] = (ecol[buf] * (rs[...] + b)).astype(BF16)
        if slot == 0:
            own = rows_of(k * CH)
            g = ecol[buf, own, :] * (rs[own, :] + b)
            gcol[own, :] = (g - eye2).astype(BF16)
        return lax.dot_general(gcol[...], imgs[...], TN, preferred_element_type=F32)

    def half(h):
        return pl.ds(h * HALF, HALF)

    def c_x3(k, h):
        return remote(xb.at[3, k, half(h)], xb.at[1, k, half(h)], sems(x3, k, h), to_x)

    def c_x2(k):
        return remote(xb.at[2, k], xb.at[0, k], sems(x2, k), to_x)

    def c_zl(k, h):
        return remote(xb.at[1, k, half(h)], rzl.at[k, half(h)], sems(zls, k, h), to_zl)

    core_buf = {7: 0, 5: 1, 6: 0, 4: 1}
    core_prev = {6: 7, 4: 5}

    def c_core(slot, k):
        return remote(cb.at[core_buf[slot], k], rc.at[slot - 4, k], sems(core, slot - 4, k), to_c)

    def c_y3(k, h):
        return remote(rc.at[3, k, half(h)], ry.at[1, k, half(h)], sems(y3, k, h), to_y)

    def c_y2(k):
        return remote(rc.at[2, k], ry.at[0, k], sems(y2, k), to_y)

    def c_zh(k, h):
        return remote(rc.at[1, k, half(h)], rzh.at[k, half(h)], sems(zhs, k, h), to_zh)

    def core_send(slot, k, buf, after):
        p = txt_chunk(slot, k, buf, after)
        if slot in core_prev:
            c_core(core_prev[slot], k).wait_send()
        cb[core_buf[slot], k] = p
        c_core(slot, k).start()

    def when(cond, fetch):
        @pl.when(cond)
        def _():
            fetch().start()

    def step(t, _):
        k = t - 1

        @pl.when(t < 4)
        def _():
            core_send(7, t, 0, lambda: get_col(3, t, 1).start())

            def row_after():
                when(t > 0, lambda: get_row(1, k, (t + 1) % 2))
                when(t == 0, lambda: get_row(3, 1, 1))

            xb[3, t] = img_chunk(3, t, t % 2, row_after)
            for h in TWO:
                c_x3(t, h).start()

            def col_after():
                when(t == 0, lambda: get_col(7, 1, 0))
                when(t > 0, lambda: get_col(5, k, 0))

            p = txt_chunk(3, t, 1, col_after)
            c_core(7, t).wait_recv()
            rc[3, t] += p
            for h in TWO:
                c_y3(t, h).start()

        @pl.when(t > 0)
        def _():
            shift = t // 4
            core_send(5, k, 0, lambda: get_col(1, k, 1).start())
            p = img_chunk(1, k, (t + 1 + shift) % 2, lambda: get_row(2, k, (t + shift) % 2).start())
            for h in TWO:
                c_x3(k, h).wait_recv()
                xb[1, k, half(h)] += p[h * HALF:h * HALF + HALF]
                c_zl(k, h).start()
            p = txt_chunk(1, k, 1, lambda: get_col(6, k, 0).start())
            c_core(5, k).wait_recv()
            for h in TWO:
                c_y3(k, h).wait_recv()
                rc[1, k, half(h)] += p[h * HALF:h * HALF + HALF] + ry[1, k, half(h)]
                c_zh(k, h).start()
            core_send(6, k, 0, lambda: get_col(2, k, 1).start())

            def row_after():
                when(t < 3, lambda: get_row(3, t + 1, (t + 1) % 2))
                when(t == 3, lambda: get_row(1, 3, 0))
                when(t == 4, lambda: get_row(0, 0, 0))

            xb[2, k] = img_chunk(2, k, (t + shift) % 2, row_after)
            c_x2(k).start()

            def col_after():
                when(t < 3, lambda: get_col(7, t + 1, 0))
                when(t == 3, lambda: get_col(5, 3, 0))
                when(t == 4, lambda: get_col(4, 0, 0))

            p = txt_chunk(2, k, 1, col_after)
            c_core(6, k).wait_recv()
            rc[2, k] += p
            c_y2(k).start()
            for i in QS:
                @pl.when(k == i)
                def _():
                    red_step(i)

        return 0

    def close(k, _):
        core_send(4, k, 0, lambda: get_col(0, k, 1).start())
        p = img_chunk(0, k, k % 2, lambda: when(k < 3, lambda: get_row(0, k + 1, (k + 1) % 2)))
        c_x2(k).wait_recv()
        xb[0, k] += p
        p = txt_chunk(0, k, 1, lambda: when(k < 3, lambda: get_col(4, k + 1, 0)))
        c_core(4, k).wait_recv()
        c_y2(k).wait_recv()
        rc[0, k] += p + ry[0, k]
        return 0

    lax.fori_loop(0, 5, step, 0)
    red_step(4)
    lax.fori_loop(0, 4, close, 0)
    loss_ref[0, 0] = jnp.sum(red[5, one(0), :]) * INV
    dt_ref[0, 0] = jnp.sum(red[5, one(1), :])

    wide = jnp.concatenate([scale] * (DIM // CH), axis=1)

    def out(n, k):
        src, dst = ((oimg, dimg_ref), (otxt, dtxt_ref))[n]
        return pltpu.make_async_copy(src.at[rows_of(k * CH), :], dst.at[rows_of(k * CH), :], s_out.at[n, k])

    def finish(k, _):
        for h in TWO:
            c_zl(k, h).wait_recv()
        oimg[rows_of(k * CH), :] = (wide * (xb[0, k] + rzl[k])).astype(BF16)
        out(0, k).start()
        for h in TWO:
            c_zh(k, h).wait_recv()
        otxt[rows_of(k * CH), :] = (wide * (rc[0, k] + rzh[k])).astype(BF16)
        out(1, k).start()
        return 0

    lax.fori_loop(0, 4, finish, 0)

    for copy in ex_col + ex_row:
        copy.wait_send()
    for k in QS:
        for copy in (g_zl, g_zh, g_x0, g_y0, g_x1, g_y1, c_x2, c_y2):
            copy(k).wait_send()
        for s in QS:
            g_c(s, k).wait_send()
        for h in TWO:
            for copy in (c_x3, c_zl, c_y3, c_zh):
                copy(k, h).wait_send()
        for slot in (6, 4):
            c_core(slot, k).wait_send()
        for n in TWO:
            out(n, k).wait()


def solution(mesh):
    spec = P(("row", "col"), None)
    smem = pl.BlockSpec(memory_space=pltpu.SMEM)
    hbm = pl.BlockSpec(memory_space=pl.ANY)
    v = pltpu.VMEM

    def dma(*shape):
        return pltpu.SemaphoreType.DMA(shape)

    chunk = (CH, DIM)
    scratch = [
        v((NI, DIM), BF16), v((NTX, DIM), BF16), v((8, BLK // CH, PIECE, CH), F32),
        v((NI, CH), F32), v((NI, CH), F32), v((8, NTX), F32), v((8, NTX), F32), v((1, NTX), F32),
        v((2, NTX // CH, CH, CH), F32), v((2, NI, CH), F32), v((CH, NTX), BF16), v((NI, CH), BF16),
        v((4, 4, *chunk), F32), v((4, *chunk), F32), v((2, 4, *chunk), F32), v((4, 4, *chunk), F32), v((2, 4, *chunk), F32), v((4, *chunk), F32),
        v((ROWS, DIM), BF16), v((ROWS, DIM), BF16),
        v((NI // CH, CH), F32), v((3, NI // CH, CH), F32), v((NTX // CH, CH), F32), v((7, NTX // CH, CH), F32), v((6, 8, CH), F32), v((5, 8, CH), F32),
        dma(2), dma(8), dma(2), dma(2), dma(2, 4),
        dma(2, 6, 4), dma(2, 4, 4), dma(2, 3), dma(2, 7), dma(2, 5),
        dma(2, 4, 2), dma(2, 4), dma(2, 4, 2), dma(2, 4, 4), dma(2, 4, 2), dma(2, 4), dma(2, 4, 2),
    ]
    shape = jax.ShapeDtypeStruct
    call = pl.pallas_call(
        kernel,
        out_shape=(shape((1, 1), F32), shape((ROWS, DIM), BF16), shape((ROWS, DIM), BF16), shape((1, 1), F32), shape((NTX // CH, NI, CH), F32)),
        in_specs=[smem, hbm, hbm],
        out_specs=(smem, hbm, hbm, smem, hbm),
        scratch_shapes=scratch,
        compiler_params=pltpu.CompilerParams(collective_id=0, has_side_effects=True, vmem_limit_bytes=67043328),
        name="clip",
    )

    def local(img, txt, log_scale):
        loss, d_img, d_txt, dt, _ = call(log_scale.reshape(1), img, txt)
        return loss[0, 0], d_img, d_txt, dt[0, 0]

    return jax.shard_map(local, mesh=mesh, in_specs=(spec, spec, P()), out_specs=(P(), spec, spec, P()), check_vma=False)
```

```python
import functools

import jax
import jax.numpy as jnp
from jax import lax
from jax.experimental import pallas as pl
from jax.experimental.pallas import tpu as pltpu
from jax.sharding import PartitionSpec as P

F32, BF16 = jnp.float32, jnp.bfloat16
MESH_ID = pl.DeviceIdType.MESH
NT = (((1,), (1,)), ((), ()))
TN = (((0,), (0,)), ((), ()))
LOG2E = 1.4426950408889634

ROWS, DIM, CH = 512, 1024, 128
NI, NTX = 4 * ROWS, 8 * ROWS
BLK, PIECE, HALF = 512, 256, 64
QS, TWO = range(4), range(2)
BATCH = 32 * ROWS
INV = 1.0 / (2 * BATCH)


def img_at(slot, k):
    if slot % 2:
        return 2 * BLK + (k // 2) * BLK + (slot // 2) * PIECE + (k % 2) * CH
    return slot // 2 * BLK + k * CH


def txt_at(slot, k):
    order = slot % 4 // 2 * 2 + slot // 4
    if slot % 2:
        return (4 + k) * BLK + order * CH
    return order * BLK + k * CH


def rows_of(start):
    return pl.ds(pl.multiple_of(start, CH), CH)


def at(i):
    return slice(i * CH, i * CH + CH)


def one(i):
    return slice(i, i + 1)


def kernel(
    t_ref, img_ref, txt_ref,
    loss_ref, dimg_ref, dtxt_ref, dt_ref, e_hbm,
    imgs, txts, est, rs, ra, cs, ca, bvec, erow, ecol, grow, gcol,
    xb, rzl, cb, rc, ry, rzh, oimg, otxt,
    rsend, rrecv, csend, crecv, red, redr,
    s_in, s_est, s_erow, s_ecol, s_out,
    ag, sib, row, colm, redm, x3, x2, zls, core, y3, y2, zhs,
):
    a = lax.axis_index("row")
    z = lax.axis_index("col")
    y, x, c = a // 4, (a // 2) % 2, a % 2
    zl, zh = z % 2, z // 2

    def dev(dx=0, dy=0, dc=0, dzl=0, dzh=0):
        yy = (1 - y) if dy else y
        xx = (1 - x) if dx else x
        cc = (1 - c) if dc else c
        l = (1 - zl) if dzl else zl
        h = (1 - zh) if dzh else zh
        return {"row": yy * 4 + xx * 2 + cc, "col": h * 2 + l}

    def row_peer(p):
        return dev(dx=p // 2, dzl=p % 2)

    def col_peer(p):
        return dev(dc=p // 4, dy=(p // 2) % 2, dzh=p % 2)

    ROW_PEERS, COL_PEERS = range(1, 4), range(1, 8)

    def remote(src, dst, sem, to):
        return pltpu.make_async_remote_copy(src_ref=src, dst_ref=dst, send_sem=sem[0], recv_sem=sem[1], device_id=to, device_id_type=MESH_ID)

    def sems(ref, *i):
        return ref.at[(0, *i)], ref.at[(1, *i)]

    in_i = pltpu.make_async_copy(img_ref, imgs.at[pl.ds(0, ROWS), :], s_in.at[0])
    in_t = pltpu.make_async_copy(txt_ref, txts.at[pl.ds(0, ROWS), :], s_in.at[1])
    in_i.start()
    in_t.start()
    barrier = pltpu.get_barrier_semaphore()
    for p in ROW_PEERS:
        pl.semaphore_signal(barrier, inc=1, device_id=row_peer(p), device_id_type=MESH_ID)
    for p in COL_PEERS:
        pl.semaphore_signal(barrier, inc=1, device_id=col_peer(p), device_id_type=MESH_ID)
    in_i.wait()
    in_t.wait()
    pl.semaphore_wait(barrier, 10)

    to_x, to_y, to_c, to_zl, to_zh = dev(dx=1), dev(dy=1), dev(dc=1), dev(dzl=1), dev(dzh=1)

    def gi(src, dst, n, to):
        return lambda k: remote(imgs.at[rows_of(img_at(src, k)), :], imgs.at[rows_of(img_at(dst, k)), :], sems(ag, n, k), to)

    def gt(src, dst, n, to):
        return lambda k: remote(txts.at[rows_of(txt_at(src, k)), :], txts.at[rows_of(txt_at(dst, k)), :], sems(ag, n, k), to)

    g_zl, g_x0, g_x1 = gi(0, 1, 0, to_zl), gi(0, 2, 1, to_x), gi(1, 3, 2, to_x)
    g_zh, g_y0, g_y1 = gt(0, 1, 3, to_zh), gt(0, 2, 4, to_y), gt(1, 3, 5, to_y)

    def g_c(s, k):
        return remote(txts.at[rows_of(txt_at(s, k)), :], txts.at[rows_of(txt_at(s + 4, k)), :], sems(sib, s, k), to_c)

    for k in QS:
        g_zl(k).start()
        g_zh(k).start()
        g_x0(k).start()
        g_y0(k).start()
        g_c(0, k).start()

    scale = jnp.exp(jnp.full((1, CH), t_ref[0], F32))
    scale_w = jnp.concatenate([scale] * (BLK // CH), axis=1) * LOG2E

    rs[...] = jnp.zeros_like(rs)
    ra[...] = jnp.zeros_like(ra)
    cs[...] = jnp.zeros_like(cs)
    ca[...] = jnp.zeros_like(ca)

    def est_copy(p, i0, j0):
        i0 = pl.multiple_of(i0, PIECE)
        return pltpu.make_async_copy(est.at[p], e_hbm.at[pl.ds(j0 // CH, BLK // CH), pl.ds(i0, PIECE), :], s_est.at[p])

    def block(m, n, p0, used=True):
        rows = BLK
        i0 = pl.multiple_of(m * BLK, BLK)
        j0 = pl.multiple_of(n * BLK, BLK)
        pieces = [(p0 + h, h * PIECE) for h in TWO]

        def drained():
            for p, r in pieces:
                est_copy(p, i0 + r, j0).wait()

        if used is True:
            drained()
        elif used is not False:
            pl.when(used)(drained)
        acc = lax.dot_general(imgs[pl.ds(i0, rows), :], txts[pl.ds(j0, BLK), :], NT, preferred_element_type=F32)
        e = jnp.exp2(acc * scale_w)
        ea = e * acc
        parts = [e[:, at(q)] for q in range(BLK // CH)]
        prods = [ea[:, at(q)] for q in range(BLK // CH)]
        for p, r in pieces:
            for q, part in enumerate(parts):
                est[p, q] = part[r:r + PIECE]
        rs[pl.ds(i0, rows), :] += sum(parts[1:], parts[0])
        ra[pl.ds(i0, rows), :] += sum(prods[1:], prods[0])
        cs[:, pl.ds(j0, BLK)] += jnp.sum(e.reshape(rows // 8, 8, BLK), axis=0)
        ca[:, pl.ds(j0, BLK)] += jnp.sum(ea.reshape(rows // 8, 8, BLK), axis=0)
        for p, r in pieces:
            est_copy(p, i0 + r, j0).start()

    def from_zl(k):
        g_zl(k).wait_recv()
        g_x1(k).start()

    def from_zh(k):
        g_zh(k).wait_recv()
        g_y1(k).start()
        g_c(1, k).start()

    def from_y(s, k):
        (g_y1 if s else g_y0)(k).wait_recv()
        g_c(2 + s, k).start()

    def have(n):
        g_c(1, n).wait_recv()
        g_c(3, n).wait_recv()

    def near(n, _):
        @pl.when(n == 0)
        def _():
            for k in QS:
                g_c(0, k).wait_recv()

        @pl.when(n == 1)
        def _():
            for h in TWO:
                from_zl(h)
                from_y(0, 2 * h)
                from_zh(h)
                from_y(0, 2 * h + 1)
            for k in QS:
                g_x0(k).wait_recv()
                g_c(2, k).wait_recv()

        @pl.when(n == 4)
        def _():
            from_zl(2)
            from_y(1, 0)
            have(0)

        late = (n + 6) // 8
        block((7 - n) // 6 * n, late * n, 0, n > 0)
        block((n + 5) // 6, 1 + late * (n - 1), 2, n > 0)
        return 0

    lax.fori_loop(0, 5, near, 0)
    from_zh(2)
    from_y(1, 1)
    for k in TWO:
        g_x1(k).wait_recv()
    have(1)

    def pairs(m):
        def body(n, _):
            for h in TWO:
                block(m, 2 * n + h, 2 * h)
            return 0

        lax.fori_loop(0, 3, body, 0)

    pairs(2)
    from_zl(3)
    from_y(1, 2)

    def both(n, _):
        @pl.when(n == 6)
        def _():
            have(2)

        for h in TWO:
            block(h, n, 2 * h)
        return 0

    lax.fori_loop(5, 7, both, 0)
    from_zh(3)
    for k in TWO:
        g_x1(2 + k).wait_recv()
    pairs(3)
    from_y(1, 3)
    for h in TWO:
        block(2 + h, 6, 2 * h)
    have(3)
    for m in QS:
        block(m, 7, 2 * m, m < 2)
    diag = jnp.zeros((CH, 128), F32)
    for k in QS:
        prod = imgs[at(k), :].astype(F32) * txts[at(k), :].astype(F32)
        for q in range(DIM // CH):
            diag += prod[:, at(q)]
    diag = jnp.sum(diag, axis=0, keepdims=True)
    for p in range(8):
        est_copy(p, 0, 0).wait()

    def get_row(slot, k, buf):
        return pltpu.make_async_copy(e_hbm.at[:, rows_of(img_at(slot, k)), :], erow.at[buf], s_erow.at[buf])

    def get_col(slot, k, buf):
        return pltpu.make_async_copy(e_hbm.at[txt_at(slot, k) // CH], ecol.at[buf], s_ecol.at[buf])

    get_row(3, 0, 0).start()
    get_col(7, 0, 0).start()

    for j in range(NTX // CH):
        csend[one(j), :] = jnp.sum(cs[:, at(j)], axis=0, keepdims=True)
    ex_col = [remote(csend, crecv.at[p - 1], sems(colm, p - 1), col_peer(p)) for p in COL_PEERS]
    for copy in ex_col:
        copy.start()
    for i in range(NI // CH):
        rsend[one(i), :] = jnp.sum(rs[at(i), :].T, axis=0, keepdims=True)
    ex_row = [remote(rsend, rrecv.at[p - 1], sems(row, p - 1), row_peer(p)) for p in ROW_PEERS]
    for copy in ex_row:
        copy.start()
    for copy in ex_col:
        copy.wait_recv()

    loss_v = -2.0 * scale * diag
    dt_v = (-2.0 * INV) * scale * diag
    dt_cols = jnp.zeros((8, CH), F32)
    for slot in range(8):
        for k in QS:
            j = txt_at(slot, k) // CH
            tot = csend[one(j), :]
            for p in COL_PEERS:
                tot += crecv[p - 1, one(txt_at(slot ^ p, k) // CH), :]
            if slot == 0:
                loss_v += jnp.log(tot)
            fac = INV / tot
            bvec[:, at(j)] = fac
            dt_cols += fac * ca[:, at(j)]
    for copy in ex_row:
        copy.wait_recv()
    dt_rows = jnp.zeros((CH, CH), F32)
    for slot in QS:
        for k in QS:
            i = img_at(slot, k) // CH
            tot = rsend[one(i), :]
            for p in ROW_PEERS:
                tot += rrecv[p - 1, one(img_at(slot ^ p, k) // CH), :]
            if slot == 0:
                loss_v += jnp.log(tot)
            fac = jnp.broadcast_to(INV / tot, (CH, CH)).T
            rs[at(i), :] = fac
            dt_rows += fac * ra[at(i), :]
    dt_v += scale * (jnp.sum(dt_rows, axis=0, keepdims=True) + jnp.sum(dt_cols, axis=0, keepdims=True))
    red[0] = jnp.concatenate([loss_v, dt_v, jnp.zeros((6, CH), F32)], axis=0)

    red_to = [to_x, to_zl, to_y, to_zh, to_c]
    ex_red = [remote(red.at[i], redr.at[i], sems(redm, i), to) for i, to in enumerate(red_to)]

    def red_step(i):
        ex_red[i].wait()
        red[i + 1] = red[i] + redr[i]
        if i + 1 < len(ex_red):
            ex_red[i + 1].start()

    ex_red[0].start()

    ri = lax.broadcasted_iota(jnp.int32, (CH, CH), 0)
    ci = lax.broadcasted_iota(jnp.int32, (CH, CH), 1)
    eye2 = jnp.where(ri == ci, 2.0 * INV, 0.0).astype(F32)

    def img_chunk(slot, k, buf, after):
        get_row(slot, k, buf).wait()
        after()
        fac = rs[rows_of(img_at(slot, k)), :]
        for j in range(NTX // CH):
            grow[:, at(j)] = (erow[buf, j] * (fac + bvec[:, at(j)])).astype(BF16)
        if slot == 0:
            j0 = pl.multiple_of(k * CH, CH)
            g = erow[buf, k] * (fac + bvec[:, pl.ds(j0, CH)])
            grow[:, pl.ds(j0, CH)] = (g - eye2).astype(BF16)
        return jnp.dot(grow[...], txts[...], preferred_element_type=F32)

    def txt_chunk(slot, k, buf, after):
        get_col(slot, k, buf).wait()
        after()
        b = bvec[:, pl.ds(pl.multiple_of(txt_at(slot, k), CH), CH)]
        gcol[...] = (ecol[buf] * (rs[...] + b)).astype(BF16)
        if slot == 0:
            own = rows_of(k * CH)
            g = ecol[buf, own, :] * (rs[own, :] + b)
            gcol[own, :] = (g - eye2).astype(BF16)
        return lax.dot_general(gcol[...], imgs[...], TN, preferred_element_type=F32)

    def half(h):
        return pl.ds(h * HALF, HALF)

    def c_x3(k, h):
        return remote(xb.at[3, k, half(h)], xb.at[1, k, half(h)], sems(x3, k, h), to_x)

    def c_x2(k):
        return remote(xb.at[2, k], xb.at[0, k], sems(x2, k), to_x)

    def c_zl(k, h):
        return remote(xb.at[1, k, half(h)], rzl.at[k, half(h)], sems(zls, k, h), to_zl)

    core_buf = {7: 0, 5: 1, 6: 0, 4: 1}
    core_prev = {6: 7, 4: 5}

    def c_core(slot, k):
        return remote(cb.at[core_buf[slot], k], rc.at[slot - 4, k], sems(core, slot - 4, k), to_c)

    def c_y3(k, h):
        return remote(rc.at[3, k, half(h)], ry.at[1, k, half(h)], sems(y3, k, h), to_y)

    def c_y2(k):
        return remote(rc.at[2, k], ry.at[0, k], sems(y2, k), to_y)

    def c_zh(k, h):
        return remote(rc.at[1, k, half(h)], rzh.at[k, half(h)], sems(zhs, k, h), to_zh)

    def core_send(slot, k, buf, after):
        p = txt_chunk(slot, k, buf, after)
        if slot in core_prev:
            c_core(core_prev[slot], k).wait_send()
        cb[core_buf[slot], k] = p
        c_core(slot, k).start()

    def when(cond, fetch):
        @pl.when(cond)
        def _():
            fetch().start()

    def step(t, _):
        k = t - 1

        @pl.when(t < 4)
        def _():
            core_send(7, t, 0, lambda: get_col(3, t, 1).start())

            def row_after():
                when(t > 0, lambda: get_row(1, k, (t + 1) % 2))
                when(t == 0, lambda: get_row(3, 1, 1))

            xb[3, t] = img_chunk(3, t, t % 2, row_after)
            for h in TWO:
                c_x3(t, h).start()

            def col_after():
                when(t == 0, lambda: get_col(7, 1, 0))
                when(t > 0, lambda: get_col(5, k, 0))

            p = txt_chunk(3, t, 1, col_after)
            c_core(7, t).wait_recv()
            rc[3, t] += p
            for h in TWO:
                c_y3(t, h).start()

        @pl.when(t > 0)
        def _():
            shift = t // 4
            core_send(5, k, 0, lambda: get_col(1, k, 1).start())
            p = img_chunk(1, k, (t + 1 + shift) % 2, lambda: get_row(2, k, (t + shift) % 2).start())
            for h in TWO:
                c_x3(k, h).wait_recv()
                xb[1, k, half(h)] += p[h * HALF:h * HALF + HALF]
                c_zl(k, h).start()
            p = txt_chunk(1, k, 1, lambda: get_col(6, k, 0).start())
            c_core(5, k).wait_recv()
            for h in TWO:
                c_y3(k, h).wait_recv()
                rc[1, k, half(h)] += p[h * HALF:h * HALF + HALF] + ry[1, k, half(h)]
                c_zh(k, h).start()
            core_send(6, k, 0, lambda: get_col(2, k, 1).start())

            def row_after():
                when(t < 3, lambda: get_row(3, t + 1, (t + 1) % 2))
                when(t == 3, lambda: get_row(1, 3, 0))
                when(t == 4, lambda: get_row(0, 0, 0))

            xb[2, k] = img_chunk(2, k, (t + shift) % 2, row_after)
            c_x2(k).start()

            def col_after():
                when(t < 3, lambda: get_col(7, t + 1, 0))
                when(t == 3, lambda: get_col(5, 3, 0))
                when(t == 4, lambda: get_col(4, 0, 0))

            p = txt_chunk(2, k, 1, col_after)
            c_core(6, k).wait_recv()
            rc[2, k] += p
            c_y2(k).start()
            for i in QS:
                @pl.when(k == i)
                def _():
                    red_step(i)

        return 0

    def close(k, _):
        core_send(4, k, 0, lambda: get_col(0, k, 1).start())
        p = img_chunk(0, k, k % 2, lambda: when(k < 3, lambda: get_row(0, k + 1, (k + 1) % 2)))
        c_x2(k).wait_recv()
        xb[0, k] += p
        p = txt_chunk(0, k, 1, lambda: when(k < 3, lambda: get_col(4, k + 1, 0)))
        c_core(4, k).wait_recv()
        c_y2(k).wait_recv()
        rc[0, k] += p + ry[0, k]
        return 0

    lax.fori_loop(0, 5, step, 0)
    red_step(4)
    lax.fori_loop(0, 4, close, 0)
    loss_ref[0, 0] = jnp.sum(red[5, one(0), :]) * INV
    dt_ref[0, 0] = jnp.sum(red[5, one(1), :])

    wide = jnp.concatenate([scale] * (DIM // CH), axis=1)

    def out(n, k):
        src, dst = ((oimg, dimg_ref), (otxt, dtxt_ref))[n]
        return pltpu.make_async_copy(src.at[rows_of(k * CH), :], dst.at[rows_of(k * CH), :], s_out.at[n, k])

    def finish(k, _):
        for h in TWO:
            c_zl(k, h).wait_recv()
        oimg[rows_of(k * CH), :] = (wide * (xb[0, k] + rzl[k])).astype(BF16)
        out(0, k).start()
        for h in TWO:
            c_zh(k, h).wait_recv()
        otxt[rows_of(k * CH), :] = (wide * (rc[0, k] + rzh[k])).astype(BF16)
        out(1, k).start()
        return 0

    lax.fori_loop(0, 4, finish, 0)

    for copy in ex_col + ex_row:
        copy.wait_send()
    for k in QS:
        for copy in (g_zl, g_zh, g_x0, g_y0, g_x1, g_y1, c_x2, c_y2):
            copy(k).wait_send()
        for s in QS:
            g_c(s, k).wait_send()
        for h in TWO:
            for copy in (c_x3, c_zl, c_y3, c_zh):
                copy(k, h).wait_send()
        for slot in (6, 4):
            c_core(slot, k).wait_send()
        for n in TWO:
            out(n, k).wait()


def solution(mesh):
    spec = P(("row", "col"), None)
    smem = pl.BlockSpec(memory_space=pltpu.SMEM)
    hbm = pl.BlockSpec(memory_space=pl.ANY)
    v = pltpu.VMEM

    def dma(*shape):
        return pltpu.SemaphoreType.DMA(shape)

    chunk = (CH, DIM)
    scratch = [
        v((NI, DIM), BF16), v((NTX, DIM), BF16), v((8, BLK // CH, PIECE, CH), F32),
        v((NI, CH), F32), v((NI, CH), F32), v((8, NTX), F32), v((8, NTX), F32), v((1, NTX), F32),
        v((2, NTX // CH, CH, CH), F32), v((2, NI, CH), F32), v((CH, NTX), BF16), v((NI, CH), BF16),
        v((4, 4, *chunk), F32), v((4, *chunk), F32), v((2, 4, *chunk), F32), v((4, 4, *chunk), F32), v((2, 4, *chunk), F32), v((4, *chunk), F32),
        v((ROWS, DIM), BF16), v((ROWS, DIM), BF16),
        v((NI // CH, CH), F32), v((3, NI // CH, CH), F32), v((NTX // CH, CH), F32), v((7, NTX // CH, CH), F32), v((6, 8, CH), F32), v((5, 8, CH), F32),
        dma(2), dma(8), dma(2), dma(2), dma(2, 4),
        dma(2, 6, 4), dma(2, 4, 4), dma(2, 3), dma(2, 7), dma(2, 5),
        dma(2, 4, 2), dma(2, 4), dma(2, 4, 2), dma(2, 4, 4), dma(2, 4, 2), dma(2, 4), dma(2, 4, 2),
    ]
    shape = jax.ShapeDtypeStruct
    call = pl.pallas_call(
        kernel,
        out_shape=(shape((1, 1), F32), shape((ROWS, DIM), BF16), shape((ROWS, DIM), BF16), shape((1, 1), F32), shape((NTX // CH, NI, CH), F32)),
        in_specs=[smem, hbm, hbm],
        out_specs=(smem, hbm, hbm, smem, hbm),
        scratch_shapes=scratch,
        compiler_params=pltpu.CompilerParams(collective_id=0, has_side_effects=True, vmem_limit_bytes=67043328),
        name="clip",
    )

    def local(img, txt, log_scale):
        loss, d_img, d_txt, dt, _ = call(log_scale.reshape(1), img, txt)
        return loss[0, 0], d_img, d_txt, dt[0, 0]

    return jax.shard_map(local, mesh=mesh, in_specs=(spec, spec, P()), out_specs=(P(), spec, spec, P()), check_vma=False)
```

```python
import functools

import jax
import jax.numpy as jnp
from jax import lax
from jax.experimental import pallas as pl
from jax.experimental.pallas import tpu as pltpu
from jax.sharding import PartitionSpec as P

F32, BF16 = jnp.float32, jnp.bfloat16
MESH_ID = pl.DeviceIdType.MESH
NT = (((1,), (1,)), ((), ()))
TN = (((0,), (0,)), ((), ()))
LOG2E = 1.4426950408889634

ROWS, DIM, CH = 512, 1024, 128
NI, NTX = 4 * ROWS, 8 * ROWS
BLK, PIECE, CUT = 512, 256, 32
QS, TWO = range(4), range(2)
HEAD, TAIL = slice(0, CUT), slice(CUT, CH)
BATCH = 32 * ROWS
INV = 1.0 / (2 * BATCH)


def img_at(slot, k):
    if slot % 2:
        return 2 * BLK + (k // 2) * BLK + (slot // 2) * PIECE + (k % 2) * CH
    return slot // 2 * BLK + k * CH


def txt_at(slot, k):
    order = slot % 4 // 2 * 2 + slot // 4
    if slot % 2:
        return (4 + k) * BLK + order * CH
    return order * BLK + k * CH


def rows_of(start):
    return pl.ds(pl.multiple_of(start, CH), CH)


def at(i):
    return slice(i * CH, i * CH + CH)


def one(i):
    return slice(i, i + 1)


def kernel(
    t_ref, img_ref, txt_ref,
    loss_ref, dimg_ref, dtxt_ref, dt_ref, e_hbm,
    imgs, txts, est, rs, ra, cs, ca, bvec, erow, ecol, grow, gcol,
    xb, rzl, cb, rc, ry, rzh, oimg, otxt, early, rz,
    rsend, rrecv, csend, crecv, red, redr,
    s_in, s_est, s_erow, s_ecol, s_out,
    ag, sib, row, colm, redm, x3, x2, zls, core, y3, y2, zhs, zf,
):
    a = lax.axis_index("row")
    z = lax.axis_index("col")
    y, x, c = a // 4, (a // 2) % 2, a % 2
    zl, zh = z % 2, z // 2

    def dev(*flip):
        yy, xx, cc, h, l = (1 - v if n in flip else v for n, v in zip(("y", "x", "c", "zh", "zl"), (y, x, c, zh, zl)))
        return {"row": yy * 4 + xx * 2 + cc, "col": h * 2 + l}

    def row_peer(p):
        return dev(*(n for i, n in enumerate(("zl", "x")) if p >> i & 1))

    def col_peer(p):
        return dev(*(n for i, n in enumerate(("zh", "y", "c")) if p >> i & 1))

    ROW_PEERS, COL_PEERS = range(1, 4), range(1, 8)

    def remote(src, dst, sem, to):
        return pltpu.make_async_remote_copy(src_ref=src, dst_ref=dst, send_sem=sem[0], recv_sem=sem[1], device_id=to, device_id_type=MESH_ID)

    def sems(ref, *i):
        return ref.at[(0, *i)], ref.at[(1, *i)]

    in_i = pltpu.make_async_copy(img_ref, imgs.at[pl.ds(0, ROWS), :], s_in.at[0])
    in_t = pltpu.make_async_copy(txt_ref, txts.at[pl.ds(0, ROWS), :], s_in.at[1])
    in_i.start()
    in_t.start()
    barrier = pltpu.get_barrier_semaphore()
    for p in ROW_PEERS:
        pl.semaphore_signal(barrier, inc=1, device_id=row_peer(p), device_id_type=MESH_ID)
    for p in COL_PEERS:
        pl.semaphore_signal(barrier, inc=1, device_id=col_peer(p), device_id_type=MESH_ID)
    in_i.wait()
    in_t.wait()
    pl.semaphore_wait(barrier, 10)

    to_x, to_y, to_c, to_zl, to_zh = (dev(n) for n in ("x", "y", "c", "zl", "zh"))

    def gi(src, dst, n, to):
        return lambda k: remote(imgs.at[rows_of(img_at(src, k)), :], imgs.at[rows_of(img_at(dst, k)), :], sems(ag, n, k), to)

    def gt(src, dst, n, to):
        return lambda k: remote(txts.at[rows_of(txt_at(src, k)), :], txts.at[rows_of(txt_at(dst, k)), :], sems(ag, n, k), to)

    g_zl, g_x0, g_x1 = gi(0, 1, 0, to_zl), gi(0, 2, 1, to_x), gi(1, 3, 2, to_x)
    g_zh, g_y0, g_y1 = gt(0, 1, 3, to_zh), gt(0, 2, 4, to_y), gt(1, 3, 5, to_y)

    def g_c(s, k):
        return remote(txts.at[rows_of(txt_at(s, k)), :], txts.at[rows_of(txt_at(s + 4, k)), :], sems(sib, s, k), to_c)

    for k in QS:
        g_zl(k).start()
        g_zh(k).start()
        g_x0(k).start()
        g_y0(k).start()
        g_c(0, k).start()

    scale = jnp.exp(jnp.full((1, CH), t_ref[0], F32))
    scale_w = jnp.concatenate([scale] * (BLK // CH), axis=1) * LOG2E

    rs[...] = jnp.zeros_like(rs)
    ra[...] = jnp.zeros_like(ra)
    cs[...] = jnp.zeros_like(cs)
    ca[...] = jnp.zeros_like(ca)

    def est_copy(p, i0, j0):
        i0 = pl.multiple_of(i0, PIECE)
        return pltpu.make_async_copy(est.at[p], e_hbm.at[pl.ds(j0 // CH, BLK // CH), pl.ds(i0, PIECE), :], s_est.at[p])

    def block(m, n, p0, used=True):
        rows = BLK
        i0 = pl.multiple_of(m * BLK, BLK)
        j0 = pl.multiple_of(n * BLK, BLK)
        pieces = [(p0 + h, h * PIECE) for h in TWO]

        def drained():
            for p, r in pieces:
                est_copy(p, i0 + r, j0).wait()

        if used is True:
            drained()
        elif used is not False:
            pl.when(used)(drained)
        acc = lax.dot_general(imgs[pl.ds(i0, rows), :], txts[pl.ds(j0, BLK), :], NT, preferred_element_type=F32)
        e = jnp.exp2(acc * scale_w)
        ea = e * acc
        parts = [e[:, at(q)] for q in range(BLK // CH)]
        prods = [ea[:, at(q)] for q in range(BLK // CH)]
        for p, r in pieces:
            for q, part in enumerate(parts):
                est[p, q] = part[r:r + PIECE]
        rs[pl.ds(i0, rows), :] += sum(parts[1:], parts[0])
        ra[pl.ds(i0, rows), :] += sum(prods[1:], prods[0])
        cs[:, pl.ds(j0, BLK)] += jnp.sum(e.reshape(rows // 8, 8, BLK), axis=0)
        ca[:, pl.ds(j0, BLK)] += jnp.sum(ea.reshape(rows // 8, 8, BLK), axis=0)
        for p, r in pieces:
            est_copy(p, i0 + r, j0).start()

    def from_zl(k):
        g_zl(k).wait_recv()
        g_x1(k).start()

    def from_zh(k):
        g_zh(k).wait_recv()
        g_y1(k).start()
        g_c(1, k).start()

    def from_y(s, k):
        (g_y1 if s else g_y0)(k).wait_recv()
        g_c(2 + s, k).start()

    def have(n):
        g_c(1, n).wait_recv()
        g_c(3, n).wait_recv()

    def near(n, _):
        @pl.when(n == 0)
        def _():
            for k in QS:
                g_c(0, k).wait_recv()

        @pl.when(n == 1)
        def _():
            for h in TWO:
                from_zl(h)
                from_y(0, 2 * h)
                from_zh(h)
                from_y(0, 2 * h + 1)
            for k in QS:
                g_x0(k).wait_recv()
                g_c(2, k).wait_recv()

        @pl.when(n == 4)
        def _():
            from_zl(2)
            from_y(1, 0)
            have(0)

        late = (n + 6) // 8
        block((7 - n) // 6 * n, late * n, 0, n > 0)
        block((n + 5) // 6, 1 + late * (n - 1), 2, n > 0)
        return 0

    lax.fori_loop(0, 5, near, 0)
    from_zh(2)
    from_y(1, 1)
    for k in TWO:
        g_x1(k).wait_recv()
    have(1)

    def pairs(m):
        def body(n, _):
            for h in TWO:
                block(m, 2 * n + h, 2 * h)
            return 0

        lax.fori_loop(0, 3, body, 0)

    pairs(2)
    from_zl(3)
    from_y(1, 2)

    def both(n, _):
        @pl.when(n == 6)
        def _():
            have(2)

        for h in TWO:
            block(h, n, 2 * h)
        return 0

    lax.fori_loop(5, 7, both, 0)
    from_zh(3)
    for k in TWO:
        g_x1(2 + k).wait_recv()
    pairs(3)
    from_y(1, 3)
    for h in TWO:
        block(2 + h, 6, 2 * h)
    have(3)
    for m in QS:
        block(m, 7, 2 * m, m < 2)
    diag = jnp.zeros((CH, 128), F32)
    for k in QS:
        prod = imgs[at(k), :].astype(F32) * txts[at(k), :].astype(F32)
        for q in range(DIM // CH):
            diag += prod[:, at(q)]
    diag = jnp.sum(diag, axis=0, keepdims=True)
    for p in range(8):
        est_copy(p, 0, 0).wait()

    def get_row(slot, k, buf):
        return pltpu.make_async_copy(e_hbm.at[:, rows_of(img_at(slot, k)), :], erow.at[buf], s_erow.at[buf])

    def get_col(slot, k, buf):
        return pltpu.make_async_copy(e_hbm.at[txt_at(slot, k) // CH], ecol.at[buf], s_ecol.at[buf])

    get_row(3, 0, 0).start()
    get_col(7, 0, 0).start()

    for j in range(NTX // CH):
        csend[one(j), :] = jnp.sum(cs[:, at(j)], axis=0, keepdims=True)
    ex_col = [remote(csend, crecv.at[p - 1], sems(colm, p - 1), col_peer(p)) for p in COL_PEERS]
    for copy in ex_col:
        copy.start()
    for i in range(NI // CH):
        rsend[one(i), :] = jnp.sum(rs[at(i), :].T, axis=0, keepdims=True)
    ex_row = [remote(rsend, rrecv.at[p - 1], sems(row, p - 1), row_peer(p)) for p in ROW_PEERS]
    for copy in ex_row:
        copy.start()
    for copy in ex_col:
        copy.wait_recv()

    loss_v = -2.0 * scale * diag
    dt_v = (-2.0 * INV) * scale * diag
    dt_cols = jnp.zeros((8, CH), F32)
    for slot in range(8):
        for k in QS:
            j = txt_at(slot, k) // CH
            tot = csend[one(j), :]
            for p in COL_PEERS:
                tot += crecv[p - 1, one(txt_at(slot ^ p, k) // CH), :]
            if slot == 0:
                loss_v += jnp.log(tot)
            fac = INV / tot
            bvec[:, at(j)] = fac
            dt_cols += fac * ca[:, at(j)]
    for copy in ex_row:
        copy.wait_recv()
    dt_rows = jnp.zeros((CH, CH), F32)
    for slot in QS:
        for k in QS:
            i = img_at(slot, k) // CH
            tot = rsend[one(i), :]
            for p in ROW_PEERS:
                tot += rrecv[p - 1, one(img_at(slot ^ p, k) // CH), :]
            if slot == 0:
                loss_v += jnp.log(tot)
            fac = jnp.broadcast_to(INV / tot, (CH, CH)).T
            rs[at(i), :] = fac
            dt_rows += fac * ra[at(i), :]
    dt_v += scale * (jnp.sum(dt_rows, axis=0, keepdims=True) + jnp.sum(dt_cols, axis=0, keepdims=True))
    red[0] = jnp.concatenate([loss_v, dt_v, jnp.zeros((6, CH), F32)], axis=0)

    red_to = [to_x, to_zl, to_y, to_zh, to_c]
    ex_red = [remote(red.at[i], redr.at[i], sems(redm, i), to) for i, to in enumerate(red_to)]

    def red_step(i):
        ex_red[i].wait()
        red[i + 1] = red[i] + redr[i]
        if i + 1 < len(ex_red):
            ex_red[i + 1].start()

    ex_red[0].start()

    ri = lax.broadcasted_iota(jnp.int32, (CH, CH), 0)
    ci = lax.broadcasted_iota(jnp.int32, (CH, CH), 1)
    eye2 = jnp.where(ri == ci, 2.0 * INV, 0.0).astype(F32)

    def img_chunk(slot, k, buf, after):
        get_row(slot, k, buf).wait()
        after()
        fac = rs[rows_of(img_at(slot, k)), :]
        for j in range(NTX // CH):
            grow[:, at(j)] = (erow[buf, j] * (fac + bvec[:, at(j)])).astype(BF16)
        if slot == 0:
            j0 = pl.multiple_of(k * CH, CH)
            g = erow[buf, k] * (fac + bvec[:, pl.ds(j0, CH)])
            grow[:, pl.ds(j0, CH)] = (g - eye2).astype(BF16)
        return jnp.dot(grow[...], txts[...], preferred_element_type=F32)

    def txt_chunk(slot, k, buf, after):
        get_col(slot, k, buf).wait()
        after()
        b = bvec[:, pl.ds(pl.multiple_of(txt_at(slot, k), CH), CH)]
        gcol[...] = (ecol[buf] * (rs[...] + b)).astype(BF16)
        if slot == 0:
            own = rows_of(k * CH)
            g = ecol[buf, own, :] * (rs[own, :] + b)
            gcol[own, :] = (g - eye2).astype(BF16)
        return lax.dot_general(gcol[...], imgs[...], TN, preferred_element_type=F32)

    def half(h):
        return TAIL if h else HEAD

    def c_x3(k, h):
        return remote(xb.at[3, k, half(h)], xb.at[1, k, half(h)], sems(x3, k, h), to_x)

    def c_x2(k):
        return remote(xb.at[2, k], xb.at[0, k], sems(x2, k), to_x)

    def c_zl(k, h):
        return remote(xb.at[1, k, half(h)], rzl.at[k, half(h)], sems(zls, k, h), to_zl)

    def c_core(slot, k):
        return remote(cb.at[slot - 4], rc.at[slot - 4, k], sems(core, slot - 4, k), to_c)

    def c_y3(k, h):
        return remote(rc.at[3, k, half(h)], ry.at[1, k, half(h)], sems(y3, k, h), to_y)

    def c_y2(k):
        return remote(rc.at[2, k], ry.at[0, k], sems(y2, k), to_y)

    def c_zh(k, h):
        return remote(rc.at[1, k, half(h)], rzh.at[k, half(h)], sems(zhs, k, h), to_zh)

    z_first = [remote(xb.at[3, 0, HEAD], rz.at[0], sems(zf, 0), to_zl), remote(rc.at[3, 0, HEAD], rz.at[1], sems(zf, 1), to_zh)]

    def when(cond, go):
        @pl.when(cond)
        def _():
            go()

    def fetch(cond, get):
        when(cond, lambda: get().start())

    def core_send(slot, k, buf, after):
        p = txt_chunk(slot, k, buf, after)
        when(k > 0, lambda: c_core(slot, k - 1).wait_send())
        cb[slot - 4] = p
        c_core(slot, k).start()

    def step(t, _):
        k = t - 1
        km = t - (t + 3) // 4
        third, shift = t // 3, t // 4
        at0, at1, at3, at4, on = t == 0, t == 1, t == 3, t == 4, t > 0

        @pl.when(t < 4)
        def _():
            core_send(7, t, 0, lambda: get_col(3, t, 1).start())

            def row_after():
                fetch(at1, lambda: get_row(2, 0, 1))
                fetch(jnp.logical_not(at1), lambda: get_row(1, km, 1 - third))

            xb[3, t] = img_chunk(3, t, third, row_after)
            when(at0, z_first[0].start)
            when(on, lambda: c_x3(t, 0).start())
            c_x3(t, 1).start()

            def col_after():
                fetch(at1, lambda: get_col(6, 0, 0))
                fetch(jnp.logical_not(at1), lambda: get_col(5, km, 0))

            p = txt_chunk(3, t, 1, col_after)
            c_core(7, t).wait_recv()
            rc[3, t] += p
            when(at0, z_first[1].start)
            when(on, lambda: c_y3(t, 0).start())
            c_y3(t, 1).start()

        @pl.when(jnp.logical_not(at1))
        def _():
            core_send(5, km, 0, lambda: get_col(1, km, 1).start())

            def row_after():
                fetch(at0, lambda: get_row(3, 1, 0))
                fetch(on, lambda: get_row(2, k, (t + shift) % 2))

            early[...] = img_chunk(1, km, 1 - third, row_after)

            @pl.when(at0)
            def _():
                xb[1, 0, HEAD] = early[HEAD]
                c_zl(0, 0).start()

            def col_after():
                fetch(at0, lambda: get_col(7, 1, 0))
                fetch(on, lambda: get_col(6, k, 0))

            p = txt_chunk(1, km, 1, col_after)
            c_core(5, km).wait_recv()
            rc[1, km] += p
            when(at0, lambda: c_zh(0, 0).start())

        def pass_zl(h):
            c_x3(k, h).wait_recv()
            xb[1, k, half(h)] += early[half(h)]
            c_zl(k, h).start()

        def pass_zh(h):
            c_y3(k, h).wait_recv()
            rc[1, k, half(h)] += ry[1, k, half(h)]
            c_zh(k, h).start()

        @pl.when(on)
        def _():
            @pl.when(t > 1)
            def _():
                pass_zl(0)
                pass_zh(0)

            pass_zl(1)
            pass_zh(1)
            core_send(6, k, 0, lambda: get_col(2, k, 1).start())

            def row_after():
                fetch(t < 3, lambda: get_row(3, t + 1, (t + 1) // 3))
                fetch(at3, lambda: get_row(1, 3, 0))
                fetch(at4, lambda: get_row(0, 0, 0))

            xb[2, k] = img_chunk(2, k, (t + shift) % 2, row_after)

            @pl.when(at1)
            def _():
                z_first[0].wait_recv()
                xb[2, 0, HEAD] += rz[0]

            c_x2(k).start()

            def col_after():
                fetch(t < 3, lambda: get_col(7, t + 1, 0))
                fetch(at3, lambda: get_col(5, 3, 0))
                fetch(at4, lambda: get_col(4, 0, 0))

            p = txt_chunk(2, k, 1, col_after)
            c_core(6, k).wait_recv()
            rc[2, k] += p

            @pl.when(at1)
            def _():
                z_first[1].wait_recv()
                rc[2, 0, HEAD] += rz[1]

            c_y2(k).start()
            for i in QS:
                @pl.when(k == i)
                def _():
                    red_step(i)

        return 0

    def close(k, _):
        core_send(4, k, 0, lambda: get_col(0, k, 1).start())
        p = img_chunk(0, k, k % 2, lambda: fetch(k < 3, lambda: get_row(0, k + 1, (k + 1) % 2)))
        c_x2(k).wait_recv()
        xb[0, k] += p
        p = txt_chunk(0, k, 1, lambda: fetch(k < 3, lambda: get_col(4, k + 1, 0)))
        c_core(4, k).wait_recv()
        c_y2(k).wait_recv()
        rc[0, k] += p + ry[0, k]
        return 0

    lax.fori_loop(0, 5, step, 0)
    red_step(4)
    lax.fori_loop(0, 4, close, 0)
    loss_ref[0, 0] = jnp.sum(red[5, one(0), :]) * INV
    dt_ref[0, 0] = jnp.sum(red[5, one(1), :])

    wide = jnp.concatenate([scale] * (DIM // CH), axis=1)

    def out(n, k):
        src, dst = ((oimg, dimg_ref), (otxt, dtxt_ref))[n]
        return pltpu.make_async_copy(src.at[rows_of(k * CH), :], dst.at[rows_of(k * CH), :], s_out.at[n, k])

    def finish(k, _):
        for h in TWO:
            c_zl(k, h).wait_recv()
        oimg[rows_of(k * CH), :] = (wide * (xb[0, k] + rzl[k])).astype(BF16)
        out(0, k).start()
        for h in TWO:
            c_zh(k, h).wait_recv()
        otxt[rows_of(k * CH), :] = (wide * (rc[0, k] + rzh[k])).astype(BF16)
        out(1, k).start()
        return 0

    lax.fori_loop(0, 4, finish, 0)

    for copy in ex_col + ex_row + z_first:
        copy.wait_send()
    for k in QS:
        for copy in (g_zl, g_zh, g_x0, g_y0, g_x1, g_y1, c_x2, c_y2):
            copy(k).wait_send()
        for s in QS:
            g_c(s, k).wait_send()
        for h in TWO:
            for copy in (c_zl, c_zh, c_x3, c_y3):
                if k + h > 0 or copy in (c_zl, c_zh):
                    copy(k, h).wait_send()
        c_core(4 + k, 3).wait_send()
        for n in TWO:
            out(n, k).wait()


def hand_over(img_ref, txt_ref, dimg_ref, dtxt_ref, buf, sem):
    parts = [(n, k) for k in TWO for n in TWO]

    def move(n, k, way):
        here = buf.at[n, pl.ds(k * PIECE, PIECE), :]
        there = ((img_ref, txt_ref), (dimg_ref, dtxt_ref))[way][n].at[pl.ds(k * PIECE, PIECE), :]
        src, dst = (here, there) if way else (there, here)
        return pltpu.make_async_copy(src, dst, sem.at[way, n, k])

    for n, k in parts:
        move(n, k, 0).start()
    for n, k in parts:
        move(n, k, 0).wait()
        move(n, k, 1).start()
    for n, k in parts:
        move(n, k, 1).wait()


def solution(mesh):
    spec = P(("row", "col"), None)
    smem = pl.BlockSpec(memory_space=pltpu.SMEM)
    hbm = pl.BlockSpec(memory_space=pl.ANY)
    v = pltpu.VMEM

    def dma(*shape):
        return pltpu.SemaphoreType.DMA(shape)

    chunk = (CH, DIM)
    scratch = [
        v((NI, DIM), BF16), v((NTX, DIM), BF16), v((8, BLK // CH, PIECE, CH), F32),
        v((NI, CH), F32), v((NI, CH), F32), v((8, NTX), F32), v((8, NTX), F32), v((1, NTX), F32),
        v((2, NTX // CH, CH, CH), F32), v((2, NI, CH), F32), v((CH, NTX), BF16), v((NI, CH), BF16),
        v((4, 4, *chunk), F32), v((4, *chunk), F32), v((4, *chunk), F32), v((4, 4, *chunk), F32), v((2, 4, *chunk), F32), v((4, *chunk), F32),
        v((ROWS, DIM), BF16), v((ROWS, DIM), BF16), v(chunk, F32), v((2, CUT, DIM), F32),
        v((NI // CH, CH), F32), v((3, NI // CH, CH), F32), v((NTX // CH, CH), F32), v((7, NTX // CH, CH), F32), v((6, 8, CH), F32), v((5, 8, CH), F32),
        dma(2), dma(8), dma(2), dma(2), dma(2, 4),
        dma(2, 6, 4), dma(2, 4, 4), dma(2, 3), dma(2, 7), dma(2, 5),
        dma(2, 4, 2), dma(2, 4), dma(2, 4, 2), dma(2, 4, 4), dma(2, 4, 2), dma(2, 4), dma(2, 4, 2), dma(2, 2),
    ]
    shape = jax.ShapeDtypeStruct
    call = pl.pallas_call(
        kernel,
        out_shape=(shape((1, 1), F32), shape((ROWS, DIM), BF16), shape((ROWS, DIM), BF16), shape((1, 1), F32), shape((NTX // CH, NI, CH), F32)),
        in_specs=[smem, hbm, hbm],
        out_specs=(smem, hbm, hbm, smem, hbm),
        scratch_shapes=scratch,
        compiler_params=pltpu.CompilerParams(collective_id=0, has_side_effects=True, vmem_limit_bytes=67043328),
        name="clip",
    )
    final = pl.pallas_call(
        hand_over,
        out_shape=(shape((ROWS, DIM), BF16), shape((ROWS, DIM), BF16)),
        in_specs=[hbm, hbm],
        out_specs=(hbm, hbm),
        scratch_shapes=[v((2, ROWS, DIM), BF16), dma(2, 2, 2)],
        name="hand_over",
    )

    def local(img, txt, log_scale):
        loss, d_img, d_txt, dt, _ = call(log_scale.reshape(1), img, txt)
        d_img, d_txt = final(d_img, d_txt)
        return loss[0, 0], d_img, d_txt, dt[0, 0]

    return jax.shard_map(local, mesh=mesh, in_specs=(spec, spec, P()), out_specs=(P(), spec, spec, P()), check_vma=False)
```

```python
import functools

import jax
import jax.numpy as jnp
from jax import lax
from jax.experimental import pallas as pl
from jax.experimental.pallas import tpu as pltpu
from jax.sharding import PartitionSpec as P

F32, BF16 = jnp.float32, jnp.bfloat16
MESH_ID = pl.DeviceIdType.MESH
NT = (((1,), (1,)), ((), ()))
TN = (((0,), (0,)), ((), ()))
LOG2E = 1.4426950408889634

ROWS, DIM, CH = 512, 1024, 128
NI, NTX = 4 * ROWS, 8 * ROWS
BLK, PIECE, CUTS = 512, 256, (0, 16, 56, CH)
QS, TWO = range(4), range(2)
PARTS = range(3)
HEAD = slice(0, CUTS[1])
BATCH = 32 * ROWS
INV = 1.0 / (2 * BATCH)


def img_at(slot, k):
    if slot % 2:
        return 2 * BLK + (k // 2) * BLK + (slot // 2) * PIECE + (k % 2) * CH
    return slot // 2 * BLK + k * CH


def txt_at(slot, k):
    order = slot % 4 // 2 * 2 + slot // 4
    if slot % 2:
        return (4 + k) * BLK + order * CH
    return order * BLK + k * CH


def rows_of(start):
    return pl.ds(pl.multiple_of(start, CH), CH)


def at(i):
    return slice(i * CH, i * CH + CH)


def one(i):
    return slice(i, i + 1)


def kernel(
    t_ref, img_ref, txt_ref,
    loss_ref, dimg_ref, dtxt_ref, dt_ref, e_hbm,
    imgs, txts, est, rs, ra, cs, ca, bvec, erow, ecol, grow, gcol,
    xb, rzl, cb, rc, ry, rzh, oimg, otxt, early, rz,
    rsend, rrecv, csend, crecv, red, redr,
    s_in, s_est, s_erow, s_ecol, s_out,
    ag, sib, row, colm, redm, x3, x2, zls, core, y3, y2, zhs, zf,
):
    a = lax.axis_index("row")
    z = lax.axis_index("col")
    y, x, c = a // 4, (a // 2) % 2, a % 2
    zl, zh = z % 2, z // 2

    def dev(*flip):
        yy, xx, cc, h, l = (1 - v if n in flip else v for n, v in zip(("y", "x", "c", "zh", "zl"), (y, x, c, zh, zl)))
        return {"row": yy * 4 + xx * 2 + cc, "col": h * 2 + l}

    def row_peer(p):
        return dev(*(n for i, n in enumerate(("zl", "x")) if p >> i & 1))

    def col_peer(p):
        return dev(*(n for i, n in enumerate(("zh", "y", "c")) if p >> i & 1))

    ROW_PEERS, COL_PEERS = range(1, 4), range(1, 8)

    def remote(src, dst, sem, to):
        return pltpu.make_async_remote_copy(src_ref=src, dst_ref=dst, send_sem=sem[0], recv_sem=sem[1], device_id=to, device_id_type=MESH_ID)

    def sems(ref, *i):
        return ref.at[(0, *i)], ref.at[(1, *i)]

    in_i = pltpu.make_async_copy(img_ref, imgs.at[pl.ds(0, ROWS), :], s_in.at[0])
    in_t = pltpu.make_async_copy(txt_ref, txts.at[pl.ds(0, ROWS), :], s_in.at[1])
    in_i.start()
    in_t.start()
    barrier = pltpu.get_barrier_semaphore()
    for p in ROW_PEERS:
        pl.semaphore_signal(barrier, inc=1, device_id=row_peer(p), device_id_type=MESH_ID)
    for p in COL_PEERS:
        pl.semaphore_signal(barrier, inc=1, device_id=col_peer(p), device_id_type=MESH_ID)
    in_i.wait()
    in_t.wait()
    pl.semaphore_wait(barrier, 10)

    to_x, to_y, to_c, to_zl, to_zh = (dev(n) for n in ("x", "y", "c", "zl", "zh"))

    def gi(src, dst, n, to):
        return lambda k: remote(imgs.at[rows_of(img_at(src, k)), :], imgs.at[rows_of(img_at(dst, k)), :], sems(ag, n, k), to)

    def gt(src, dst, n, to):
        return lambda k: remote(txts.at[rows_of(txt_at(src, k)), :], txts.at[rows_of(txt_at(dst, k)), :], sems(ag, n, k), to)

    g_zl, g_x0, g_x1 = gi(0, 1, 0, to_zl), gi(0, 2, 1, to_x), gi(1, 3, 2, to_x)
    g_zh, g_y0, g_y1 = gt(0, 1, 3, to_zh), gt(0, 2, 4, to_y), gt(1, 3, 5, to_y)

    def g_c(s, k):
        return remote(txts.at[rows_of(txt_at(s, k)), :], txts.at[rows_of(txt_at(s + 4, k)), :], sems(sib, s, k), to_c)

    for k in QS:
        g_zl(k).start()
        g_zh(k).start()
        g_x0(k).start()
        g_y0(k).start()
        g_c(0, k).start()

    scale = jnp.exp(jnp.full((1, CH), t_ref[0], F32))
    scale_w = jnp.concatenate([scale] * (BLK // CH), axis=1) * LOG2E

    rs[...] = jnp.zeros_like(rs)
    ra[...] = jnp.zeros_like(ra)
    cs[...] = jnp.zeros_like(cs)
    ca[...] = jnp.zeros_like(ca)

    def est_copy(p, i0, j0):
        i0 = pl.multiple_of(i0, PIECE)
        return pltpu.make_async_copy(est.at[p], e_hbm.at[pl.ds(j0 // CH, BLK // CH), pl.ds(i0, PIECE), :], s_est.at[p])

    def block(m, n, p0, used=True):
        rows = BLK
        i0 = pl.multiple_of(m * BLK, BLK)
        j0 = pl.multiple_of(n * BLK, BLK)
        pieces = [(p0 + h, h * PIECE) for h in TWO]

        def drained():
            for p, r in pieces:
                est_copy(p, i0 + r, j0).wait()

        if used is True:
            drained()
        elif used is not False:
            pl.when(used)(drained)
        acc = lax.dot_general(imgs[pl.ds(i0, rows), :], txts[pl.ds(j0, BLK), :], NT, preferred_element_type=F32)
        e = jnp.exp2(acc * scale_w)
        ea = e * acc
        parts = [e[:, at(q)] for q in range(BLK // CH)]
        prods = [ea[:, at(q)] for q in range(BLK // CH)]
        for p, r in pieces:
            for q, part in enumerate(parts):
                est[p, q] = part[r:r + PIECE]
        rs[pl.ds(i0, rows), :] += sum(parts[1:], parts[0])
        ra[pl.ds(i0, rows), :] += sum(prods[1:], prods[0])
        cs[:, pl.ds(j0, BLK)] += jnp.sum(e.reshape(rows // 8, 8, BLK), axis=0)
        ca[:, pl.ds(j0, BLK)] += jnp.sum(ea.reshape(rows // 8, 8, BLK), axis=0)
        for p, r in pieces:
            est_copy(p, i0 + r, j0).start()

    def from_zl(k):
        g_zl(k).wait_recv()
        g_x1(k).start()

    def from_zh(k):
        g_zh(k).wait_recv()
        g_y1(k).start()
        g_c(1, k).start()

    def from_y(s, k):
        (g_y1 if s else g_y0)(k).wait_recv()
        g_c(2 + s, k).start()

    def have(n):
        g_c(1, n).wait_recv()
        g_c(3, n).wait_recv()

    def near(n, _):
        @pl.when(n == 0)
        def _():
            for k in QS:
                g_c(0, k).wait_recv()

        @pl.when(n == 1)
        def _():
            for h in TWO:
                from_zl(h)
                from_y(0, 2 * h)
                from_zh(h)
                from_y(0, 2 * h + 1)
            for k in QS:
                g_x0(k).wait_recv()
                g_c(2, k).wait_recv()

        @pl.when(n == 4)
        def _():
            from_zl(2)
            from_y(1, 0)
            have(0)

        late = (n + 6) // 8
        block((7 - n) // 6 * n, late * n, 0, n > 0)
        block((n + 5) // 6, 1 + late * (n - 1), 2, n > 0)
        return 0

    lax.fori_loop(0, 5, near, 0)
    from_zh(2)
    from_y(1, 1)
    for k in TWO:
        g_x1(k).wait_recv()
    have(1)

    def pairs(m):
        def body(n, _):
            for h in TWO:
                block(m, 2 * n + h, 2 * h)
            return 0

        lax.fori_loop(0, 3, body, 0)

    pairs(2)
    from_zl(3)
    from_y(1, 2)

    def both(n, _):
        @pl.when(n == 6)
        def _():
            have(2)

        for h in TWO:
            block(h, n, 2 * h)
        return 0

    lax.fori_loop(5, 7, both, 0)
    from_zh(3)
    for k in TWO:
        g_x1(2 + k).wait_recv()
    pairs(3)
    from_y(1, 3)
    for h in TWO:
        block(2 + h, 6, 2 * h)
    have(3)
    for m in QS:
        block(m, 7, 2 * m, m < 2)
    diag = jnp.zeros((CH, 128), F32)
    for k in QS:
        prod = imgs[at(k), :].astype(F32) * txts[at(k), :].astype(F32)
        for q in range(DIM // CH):
            diag += prod[:, at(q)]
    diag = jnp.sum(diag, axis=0, keepdims=True)
    for p in range(8):
        est_copy(p, 0, 0).wait()

    def get_row(slot, k, buf):
        return pltpu.make_async_copy(e_hbm.at[:, rows_of(img_at(slot, k)), :], erow.at[buf], s_erow.at[buf])

    def get_col(slot, k, buf):
        return pltpu.make_async_copy(e_hbm.at[txt_at(slot, k) // CH], ecol.at[buf], s_ecol.at[buf])

    get_row(3, 0, 0).start()
    get_col(7, 0, 0).start()

    for j in range(NTX // CH):
        csend[one(j), :] = jnp.sum(cs[:, at(j)], axis=0, keepdims=True)
    ex_col = [remote(csend, crecv.at[p - 1], sems(colm, p - 1), col_peer(p)) for p in COL_PEERS]
    for copy in ex_col:
        copy.start()
    for i in range(NI // CH):
        rsend[one(i), :] = jnp.sum(rs[at(i), :].T, axis=0, keepdims=True)
    ex_row = [remote(rsend, rrecv.at[p - 1], sems(row, p - 1), row_peer(p)) for p in ROW_PEERS]
    for copy in ex_row:
        copy.start()
    for copy in ex_col:
        copy.wait_recv()

    loss_v = -2.0 * scale * diag
    dt_v = (-2.0 * INV) * scale * diag
    dt_cols = jnp.zeros((8, CH), F32)
    for slot in range(8):
        for k in QS:
            j = txt_at(slot, k) // CH
            tot = csend[one(j), :]
            for p in COL_PEERS:
                tot += crecv[p - 1, one(txt_at(slot ^ p, k) // CH), :]
            if slot == 0:
                loss_v += jnp.log(tot)
            fac = INV / tot
            bvec[:, at(j)] = fac
            dt_cols += fac * ca[:, at(j)]
    for copy in ex_row:
        copy.wait_recv()
    dt_rows = jnp.zeros((CH, CH), F32)
    for slot in QS:
        for k in QS:
            i = img_at(slot, k) // CH
            tot = rsend[one(i), :]
            for p in ROW_PEERS:
                tot += rrecv[p - 1, one(img_at(slot ^ p, k) // CH), :]
            if slot == 0:
                loss_v += jnp.log(tot)
            fac = jnp.broadcast_to(INV / tot, (CH, CH)).T
            rs[at(i), :] = fac
            dt_rows += fac * ra[at(i), :]
    dt_v += scale * (jnp.sum(dt_rows, axis=0, keepdims=True) + jnp.sum(dt_cols, axis=0, keepdims=True))
    red[0] = jnp.concatenate([loss_v, dt_v, jnp.zeros((6, CH), F32)], axis=0)

    red_to = [to_x, to_zl, to_y, to_zh, to_c]
    ex_red = [remote(red.at[i], redr.at[i], sems(redm, i), to) for i, to in enumerate(red_to)]

    def red_step(i):
        ex_red[i].wait()
        red[i + 1] = red[i] + redr[i]
        if i + 1 < len(ex_red):
            ex_red[i + 1].start()

    ex_red[0].start()

    ri = lax.broadcasted_iota(jnp.int32, (CH, CH), 0)
    ci = lax.broadcasted_iota(jnp.int32, (CH, CH), 1)
    eye2 = jnp.where(ri == ci, 2.0 * INV, 0.0).astype(F32)

    def img_chunk(slot, k, buf, after):
        get_row(slot, k, buf).wait()
        after()
        fac = rs[rows_of(img_at(slot, k)), :]
        for j in range(NTX // CH):
            grow[:, at(j)] = (erow[buf, j] * (fac + bvec[:, at(j)])).astype(BF16)
        if slot == 0:
            j0 = pl.multiple_of(k * CH, CH)
            g = erow[buf, k] * (fac + bvec[:, pl.ds(j0, CH)])
            grow[:, pl.ds(j0, CH)] = (g - eye2).astype(BF16)
        return jnp.dot(grow[...], txts[...], preferred_element_type=F32)

    def txt_chunk(slot, k, buf, after):
        get_col(slot, k, buf).wait()
        after()
        b = bvec[:, pl.ds(pl.multiple_of(txt_at(slot, k), CH), CH)]
        gcol[...] = (ecol[buf] * (rs[...] + b)).astype(BF16)
        if slot == 0:
            own = rows_of(k * CH)
            g = ecol[buf, own, :] * (rs[own, :] + b)
            gcol[own, :] = (g - eye2).astype(BF16)
        return lax.dot_general(gcol[...], imgs[...], TN, preferred_element_type=F32)

    def half(h):
        return slice(CUTS[h], CUTS[h + 1])

    def c_x3(k, h):
        return remote(xb.at[3, k, half(h)], xb.at[1, k, half(h)], sems(x3, k, h), to_x)

    def c_x2(k):
        return remote(xb.at[2, k], xb.at[0, k], sems(x2, k), to_x)

    def c_zl(k, h):
        return remote(xb.at[1, k, half(h)], rzl.at[k, half(h)], sems(zls, k, h), to_zl)

    def c_core(slot, k):
        return remote(cb.at[slot - 4], rc.at[slot - 4, k], sems(core, slot - 4, k), to_c)

    def c_y3(k, h):
        return remote(rc.at[3, k, half(h)], ry.at[1, k, half(h)], sems(y3, k, h), to_y)

    def c_y2(k):
        return remote(rc.at[2, k], ry.at[0, k], sems(y2, k), to_y)

    def c_zh(k, h):
        return remote(rc.at[1, k, half(h)], rzh.at[k, half(h)], sems(zhs, k, h), to_zh)

    z_first = [remote(xb.at[3, 0, HEAD], rz.at[0], sems(zf, 0), to_zl), remote(rc.at[3, 0, HEAD], rz.at[1], sems(zf, 1), to_zh)]

    def when(cond, go):
        @pl.when(cond)
        def _():
            go()

    def fetch(cond, get):
        when(cond, lambda: get().start())

    def core_send(slot, k, buf, after):
        p = txt_chunk(slot, k, buf, after)
        when(k > 0, lambda: c_core(slot, k - 1).wait_send())
        cb[slot - 4] = p
        c_core(slot, k).start()

    def pass_zl(k, h):
        c_x3(k, h).wait_recv()
        xb[1, k, half(h)] += early[half(h)]
        c_zl(k, h).start()

    def pass_zh(k, h):
        c_y3(k, h).wait_recv()
        rc[1, k, half(h)] += ry[1, k, half(h)]
        c_zh(k, h).start()

    def step(t, _):
        k = t - 1
        km = t - (t + 3) // 4
        third, shift = t // 3, t // 4
        at0, at1, at3, at4, on = t == 0, t == 1, t == 3, t == 4, t > 0

        @pl.when(t < 4)
        def _():
            core_send(7, t, 0, lambda: get_col(3, t, 1).start())

            def row_after():
                fetch(at1, lambda: get_row(2, 0, 1))
                fetch(jnp.logical_not(at1), lambda: get_row(1, km, 1 - third))

            xb[3, t] = img_chunk(3, t, third, row_after)
            when(at0, z_first[0].start)
            when(on, lambda: c_x3(t, 0).start())
            for h in TWO:
                c_x3(t, h + 1).start()

            def col_after():
                fetch(at1, lambda: get_col(6, 0, 0))
                fetch(jnp.logical_not(at1), lambda: get_col(5, km, 0))

            p = txt_chunk(3, t, 1, col_after)
            c_core(7, t).wait_recv()
            rc[3, t] += p
            when(at0, z_first[1].start)
            when(on, lambda: c_y3(t, 0).start())
            for h in TWO:
                c_y3(t, h + 1).start()

        @pl.when(jnp.logical_not(at1))
        def _():
            core_send(5, km, 0, lambda: get_col(1, km, 1).start())

            def row_after():
                fetch(at0, lambda: get_row(3, 1, 0))
                fetch(on, lambda: get_row(2, k, (t + shift) % 2))

            early[...] = img_chunk(1, km, 1 - third, row_after)

            @pl.when(at0)
            def _():
                xb[1, 0, HEAD] = early[HEAD]
                c_zl(0, 0).start()

            def col_after():
                fetch(at0, lambda: get_col(7, 1, 0))
                fetch(on, lambda: get_col(6, k, 0))

            p = txt_chunk(1, km, 1, col_after)
            c_core(5, km).wait_recv()
            rc[1, km] += p
            when(at0, lambda: c_zh(0, 0).start())

            @pl.when(on)
            def _():
                pass_zl(km, 0)
                pass_zh(km, 0)

            pass_zl(km, 1)
            pass_zh(km, 1)

        @pl.when(on)
        def _():
            pass_zl(k, 2)
            pass_zh(k, 2)
            core_send(6, k, 0, lambda: get_col(2, k, 1).start())

            def row_after():
                fetch(t < 3, lambda: get_row(3, t + 1, (t + 1) // 3))
                fetch(at3, lambda: get_row(1, 3, 0))
                fetch(at4, lambda: get_row(0, 0, 0))

            xb[2, k] = img_chunk(2, k, (t + shift) % 2, row_after)

            @pl.when(at1)
            def _():
                z_first[0].wait_recv()
                xb[2, 0, HEAD] += rz[0]

            c_x2(k).start()

            def col_after():
                fetch(t < 3, lambda: get_col(7, t + 1, 0))
                fetch(at3, lambda: get_col(5, 3, 0))
                fetch(at4, lambda: get_col(4, 0, 0))

            p = txt_chunk(2, k, 1, col_after)
            c_core(6, k).wait_recv()
            rc[2, k] += p

            @pl.when(at1)
            def _():
                z_first[1].wait_recv()
                rc[2, 0, HEAD] += rz[1]

            c_y2(k).start()
            for i in QS:
                @pl.when(k == i)
                def _():
                    red_step(i)

        return 0

    def close(k, _):
        core_send(4, k, 0, lambda: get_col(0, k, 1).start())
        p = img_chunk(0, k, k % 2, lambda: fetch(k < 3, lambda: get_row(0, k + 1, (k + 1) % 2)))
        c_x2(k).wait_recv()
        xb[0, k] += p
        p = txt_chunk(0, k, 1, lambda: fetch(k < 3, lambda: get_col(4, k + 1, 0)))
        c_core(4, k).wait_recv()
        c_y2(k).wait_recv()
        rc[0, k] += p + ry[0, k]
        return 0

    lax.fori_loop(0, 5, step, 0)
    red_step(4)
    lax.fori_loop(0, 4, close, 0)
    loss_ref[0, 0] = jnp.sum(red[5, one(0), :]) * INV
    dt_ref[0, 0] = jnp.sum(red[5, one(1), :])

    wide = jnp.concatenate([scale] * (DIM // CH), axis=1)

    def out(n, k):
        src, dst = ((oimg, dimg_ref), (otxt, dtxt_ref))[n]
        return pltpu.make_async_copy(src.at[rows_of(k * CH), :], dst.at[rows_of(k * CH), :], s_out.at[n, k])

    def finish(k, _):
        for h in PARTS:
            c_zl(k, h).wait_recv()
        oimg[rows_of(k * CH), :] = (wide * (xb[0, k] + rzl[k])).astype(BF16)
        out(0, k).start()
        for h in PARTS:
            c_zh(k, h).wait_recv()
        otxt[rows_of(k * CH), :] = (wide * (rc[0, k] + rzh[k])).astype(BF16)
        out(1, k).start()
        return 0

    for copy in ex_col + ex_row + z_first:
        copy.wait_send()
    for k in QS:
        for copy in (g_zl, g_zh, g_x0, g_y0, g_x1, g_y1, c_x2, c_y2):
            copy(k).wait_send()
        for s in QS:
            g_c(s, k).wait_send()
        for h in PARTS:
            if k + h > 0:
                c_x3(k, h).wait_send()
                c_y3(k, h).wait_send()
        c_core(4 + k, 3).wait_send()
    lax.fori_loop(0, 4, finish, 0)

    for k in QS:
        for h in PARTS:
            for copy in (c_zl, c_zh):
                copy(k, h).wait_send()
        for n in TWO:
            out(n, k).wait()


def hand_over(img_ref, txt_ref, dimg_ref, dtxt_ref, buf, sem):
    parts = [(n, k) for k in TWO for n in TWO]

    def move(n, k, way):
        here = buf.at[n, pl.ds(k * PIECE, PIECE), :]
        there = ((img_ref, txt_ref), (dimg_ref, dtxt_ref))[way][n].at[pl.ds(k * PIECE, PIECE), :]
        src, dst = (here, there) if way else (there, here)
        return pltpu.make_async_copy(src, dst, sem.at[way, n, k])

    for n, k in parts:
        move(n, k, 0).start()
    for n, k in parts:
        move(n, k, 0).wait()
        move(n, k, 1).start()
    for n, k in parts:
        move(n, k, 1).wait()


def solution(mesh):
    spec = P(("row", "col"), None)
    smem = pl.BlockSpec(memory_space=pltpu.SMEM)
    hbm = pl.BlockSpec(memory_space=pl.ANY)
    v = pltpu.VMEM

    def dma(*shape):
        return pltpu.SemaphoreType.DMA(shape)

    chunk = (CH, DIM)
    scratch = [
        v((NI, DIM), BF16), v((NTX, DIM), BF16), v((8, BLK // CH, PIECE, CH), F32),
        v((NI, CH), F32), v((NI, CH), F32), v((8, NTX), F32), v((8, NTX), F32), v((1, NTX), F32),
        v((2, NTX // CH, CH, CH), F32), v((2, NI, CH), F32), v((CH, NTX), BF16), v((NI, CH), BF16),
        v((4, 4, *chunk), F32), v((4, *chunk), F32), v((4, *chunk), F32), v((4, 4, *chunk), F32), v((2, 4, *chunk), F32), v((4, *chunk), F32),
        v((ROWS, DIM), BF16), v((ROWS, DIM), BF16), v(chunk, F32), v((2, CUTS[1], DIM), F32),
        v((NI // CH, CH), F32), v((3, NI // CH, CH), F32), v((NTX // CH, CH), F32), v((7, NTX // CH, CH), F32), v((6, 8, CH), F32), v((5, 8, CH), F32),
        dma(2), dma(8), dma(2), dma(2), dma(2, 4),
        dma(2, 6, 4), dma(2, 4, 4), dma(2, 3), dma(2, 7), dma(2, 5),
        dma(2, 4, 3), dma(2, 4), dma(2, 4, 3), dma(2, 4, 4), dma(2, 4, 3), dma(2, 4), dma(2, 4, 3), dma(2, 2),
    ]
    shape = jax.ShapeDtypeStruct
    call = pl.pallas_call(
        kernel,
        out_shape=(shape((1, 1), F32), shape((ROWS, DIM), BF16), shape((ROWS, DIM), BF16), shape((1, 1), F32), shape((NTX // CH, NI, CH), F32)),
        in_specs=[smem, hbm, hbm],
        out_specs=(smem, hbm, hbm, smem, hbm),
        scratch_shapes=scratch,
        compiler_params=pltpu.CompilerParams(collective_id=0, has_side_effects=True, vmem_limit_bytes=67043328),
        name="clip",
    )
    final = pl.pallas_call(
        hand_over,
        out_shape=(shape((ROWS, DIM), BF16), shape((ROWS, DIM), BF16)),
        in_specs=[hbm, hbm],
        out_specs=(hbm, hbm),
        scratch_shapes=[v((2, ROWS, DIM), BF16), dma(2, 2, 2)],
        name="hand_over",
    )

    def local(img, txt, log_scale):
        loss, d_img, d_txt, dt, _ = call(log_scale.reshape(1), img, txt)
        d_img, d_txt = final(d_img, d_txt)
        return loss[0, 0], d_img, d_txt, dt[0, 0]

    return jax.shard_map(local, mesh=mesh, in_specs=(spec, spec, P()), out_specs=(P(), spec, spec, P()), check_vma=False)
```

```python
import functools

import jax
import jax.numpy as jnp
from jax import lax
from jax.experimental import pallas as pl
from jax.experimental.pallas import tpu as pltpu
from jax.sharding import PartitionSpec as P

F32, BF16 = jnp.float32, jnp.bfloat16
MESH_ID = pl.DeviceIdType.MESH
NT = (((1,), (1,)), ((), ()))
TN = (((0,), (0,)), ((), ()))
LOG2E = 1.4426950408889634

ROWS, DIM, CH = 512, 1024, 128
NI, NTX = 4 * ROWS, 8 * ROWS
BLK, PIECE, CUTS = 512, 256, (0, 16, 56, CH)
QS, TWO = range(4), range(2)
PARTS = range(3)
HEAD = slice(0, CUTS[1])
BATCH = 32 * ROWS
INV = 1.0 / (2 * BATCH)


def img_at(slot, k):
    if slot % 2:
        return 2 * BLK + (k // 2) * BLK + (slot // 2) * PIECE + (k % 2) * CH
    return slot // 2 * BLK + k * CH


def txt_at(slot, k):
    order = slot % 4 // 2 * 2 + slot // 4
    if slot % 2:
        return (4 + k) * BLK + order * CH
    return order * BLK + k * CH


def rows_of(start):
    return pl.ds(pl.multiple_of(start, CH), CH)


def at(i):
    return slice(i * CH, i * CH + CH)


def one(i):
    return slice(i, i + 1)


def kernel(
    t_ref, img_ref, txt_ref,
    loss_ref, dimg_ref, dtxt_ref, dt_ref, e_hbm,
    imgs, txts, est, rs, ra, cs, ca, bvec, erow, ecol, grow, gcol,
    xb, rzl, cb, rc, ry, rzh, oimg, otxt, early, rz,
    rsend, rrecv, csend, crecv, red, redr,
    s_in, s_est, s_erow, s_ecol, s_out,
    ag, sib, row, colm, redm, x3, x2, zls, core, y3, y2, zhs, zf,
):
    a = lax.axis_index("row")
    z = lax.axis_index("col")
    y, x, c = a // 4, (a // 2) % 2, a % 2
    zl, zh = z % 2, z // 2

    def dev(*flip):
        yy, xx, cc, h, l = (1 - v if n in flip else v for n, v in zip(("y", "x", "c", "zh", "zl"), (y, x, c, zh, zl)))
        return {"row": yy * 4 + xx * 2 + cc, "col": h * 2 + l}

    def row_peer(p):
        return dev(*(n for i, n in enumerate(("zl", "x")) if p >> i & 1))

    def col_peer(p):
        return dev(*(n for i, n in enumerate(("zh", "y", "c")) if p >> i & 1))

    ROW_PEERS, COL_PEERS = range(1, 4), range(1, 8)

    def remote(src, dst, sem, to):
        return pltpu.make_async_remote_copy(src_ref=src, dst_ref=dst, send_sem=sem[0], recv_sem=sem[1], device_id=to, device_id_type=MESH_ID)

    def sems(ref, *i):
        return ref.at[(0, *i)], ref.at[(1, *i)]

    in_i = pltpu.make_async_copy(img_ref, imgs.at[pl.ds(0, ROWS), :], s_in.at[0])
    in_t = pltpu.make_async_copy(txt_ref, txts.at[pl.ds(0, ROWS), :], s_in.at[1])
    in_i.start()
    in_t.start()
    barrier = pltpu.get_barrier_semaphore()
    for p in ROW_PEERS:
        pl.semaphore_signal(barrier, inc=1, device_id=row_peer(p), device_id_type=MESH_ID)
    for p in COL_PEERS:
        pl.semaphore_signal(barrier, inc=1, device_id=col_peer(p), device_id_type=MESH_ID)
    in_i.wait()
    in_t.wait()
    pl.semaphore_wait(barrier, 10)

    to_x, to_y, to_c, to_zl, to_zh = (dev(n) for n in ("x", "y", "c", "zl", "zh"))

    def gi(src, dst, n, to):
        return lambda k: remote(imgs.at[rows_of(img_at(src, k)), :], imgs.at[rows_of(img_at(dst, k)), :], sems(ag, n, k), to)

    def gt(src, dst, n, to):
        return lambda k: remote(txts.at[rows_of(txt_at(src, k)), :], txts.at[rows_of(txt_at(dst, k)), :], sems(ag, n, k), to)

    g_zl, g_x0, g_x1 = gi(0, 1, 0, to_zl), gi(0, 2, 1, to_x), gi(1, 3, 2, to_x)
    g_zh, g_y0, g_y1 = gt(0, 1, 3, to_zh), gt(0, 2, 4, to_y), gt(1, 3, 5, to_y)

    def g_c(s, k):
        return remote(txts.at[rows_of(txt_at(s, k)), :], txts.at[rows_of(txt_at(s + 4, k)), :], sems(sib, s, k), to_c)

    for k in QS:
        g_zl(k).start()
        g_zh(k).start()
        g_x0(k).start()
        g_y0(k).start()
        g_c(0, k).start()

    scale = jnp.exp(jnp.full((1, CH), t_ref[0], F32))
    scale_w = jnp.concatenate([scale] * (BLK // CH), axis=1) * LOG2E

    rs[...] = jnp.zeros_like(rs)
    ra[...] = jnp.zeros_like(ra)
    cs[...] = jnp.zeros_like(cs)
    ca[...] = jnp.zeros_like(ca)

    def est_copy(p, i0, j0):
        i0 = pl.multiple_of(i0, PIECE)
        return pltpu.make_async_copy(est.at[p], e_hbm.at[pl.ds(j0 // CH, BLK // CH), pl.ds(i0, PIECE), :], s_est.at[p])

    def block(r, n, rows, p0, used=True):
        i0 = pl.multiple_of(r * PIECE, PIECE)
        j0 = pl.multiple_of(n * BLK, BLK)
        pieces = [(p0 + h, h * PIECE) for h in range(rows // PIECE)]

        def drained():
            for p, r in pieces:
                est_copy(p, i0 + r, j0).wait()

        if used is True:
            drained()
        elif used is not False:
            pl.when(used)(drained)
        acc = lax.dot_general(imgs[pl.ds(i0, rows), :], txts[pl.ds(j0, BLK), :], NT, preferred_element_type=F32)
        e = jnp.exp2(acc * scale_w)
        ea = e * acc
        parts = [e[:, at(q)] for q in range(BLK // CH)]
        prods = [ea[:, at(q)] for q in range(BLK // CH)]
        for p, r in pieces:
            for q, part in enumerate(parts):
                est[p, q] = part[r:r + PIECE]
        rs[pl.ds(i0, rows), :] += sum(parts[1:], parts[0])
        ra[pl.ds(i0, rows), :] += sum(prods[1:], prods[0])
        cs[:, pl.ds(j0, BLK)] += jnp.sum(e.reshape(rows // 8, 8, BLK), axis=0)
        ca[:, pl.ds(j0, BLK)] += jnp.sum(ea.reshape(rows // 8, 8, BLK), axis=0)
        for p, r in pieces:
            est_copy(p, i0 + r, j0).start()

    def from_zl(k):
        g_zl(k).wait_recv()
        g_x1(k).start()

    def from_zh(k):
        g_zh(k).wait_recv()
        g_y1(k).start()
        g_c(1, k).start()

    def from_y(s, k):
        (g_y1 if s else g_y0)(k).wait_recv()
        g_c(2 + s, k).start()

    def have(n):
        g_c(1, n).wait_recv()
        g_c(3, n).wait_recv()

    def whole(m, n, p0, used=True):
        block(2 * m, n, BLK, p0, used)

    def run(r, first, count):
        def body(i, _):
            for h in TWO:
                block(r, 2 * (first + i) + h, PIECE, 2 * (i % 2) + h)
            return 0

        lax.fori_loop(0, count, body, 0)

    def near(n, _):
        @pl.when(n == 0)
        def _():
            for k in QS:
                g_c(0, k).wait_recv()

        @pl.when(n == 1)
        def _():
            for h in TWO:
                from_zl(h)
                from_y(0, 2 * h)
                from_zh(h)
                from_y(0, 2 * h + 1)
            for k in QS:
                g_x0(k).wait_recv()
                g_c(2, k).wait_recv()

        late = n // 2
        whole(n % 2 * (1 - late), late * n, 0, n > 0)
        whole((n + 2) // 3, 1 + late * (n - 1), 2, n > 0)
        return 0

    diag = jnp.zeros((CH, 128), F32)
    for k in QS:
        prod = imgs[at(k), :].astype(F32) * txts[at(k), :].astype(F32)
        for q in range(DIM // CH):
            diag += prod[:, at(q)]
    diag = jnp.sum(diag, axis=0, keepdims=True)
    lax.fori_loop(0, 4, near, 0)
    run(4, 0, 2)
    from_zl(2)
    from_y(1, 0)
    have(0)
    for m in TWO:
        whole(m, 4, 2 * m)
    from_zh(2)
    from_y(1, 1)
    for k in TWO:
        g_x1(k).wait_recv()
    run(5, 0, 2)
    have(1)
    for m in TWO:
        whole(2, 4 + m, 2 * m)
    for m in TWO:
        whole(m, 5, 2 * m)
    from_zl(3)
    from_y(1, 2)
    run(6, 0, 1)
    from_zh(3)
    have(2)
    for m in range(3):
        whole(m, 6, 2 * m % 4)
    run(6, 1, 2)
    block(6, 6, PIECE, 0)
    for k in TWO:
        g_x1(2 + k).wait_recv()
    from_y(1, 3)
    run(7, 0, 3)
    block(7, 6, PIECE, 1)
    have(3)
    for m in QS:
        whole(m, 7, 2 * m, m < 2)

    for j in range(NTX // CH):
        csend[one(j), :] = jnp.sum(cs[:, at(j)], axis=0, keepdims=True)
    ex_col = [remote(csend, crecv.at[p - 1], sems(colm, p - 1), col_peer(p)) for p in COL_PEERS]
    for copy in ex_col:
        copy.start()
    for i in range(NI // CH):
        rsend[one(i), :] = jnp.sum(rs[at(i), :].T, axis=0, keepdims=True)
    ex_row = [remote(rsend, rrecv.at[p - 1], sems(row, p - 1), row_peer(p)) for p in ROW_PEERS]
    for copy in ex_row:
        copy.start()

    for p in range(8):
        est_copy(p, 0, 0).wait()

    def get_row(slot, k, buf):
        return pltpu.make_async_copy(e_hbm.at[:, rows_of(img_at(slot, k)), :], erow.at[buf], s_erow.at[buf])

    def get_col(slot, k, buf):
        return pltpu.make_async_copy(e_hbm.at[txt_at(slot, k) // CH], ecol.at[buf], s_ecol.at[buf])

    get_row(3, 0, 0).start()
    get_col(7, 0, 0).start()
    for copy in ex_col:
        copy.wait_recv()

    loss_v = -2.0 * scale * diag
    dt_v = (-2.0 * INV) * scale * diag
    dt_cols = jnp.zeros((8, CH), F32)
    for slot in range(8):
        for k in QS:
            j = txt_at(slot, k) // CH
            tot = csend[one(j), :]
            for p in COL_PEERS:
                tot += crecv[p - 1, one(txt_at(slot ^ p, k) // CH), :]
            if slot == 0:
                loss_v += jnp.log(tot)
            fac = INV / tot
            bvec[:, at(j)] = fac
            dt_cols += fac * ca[:, at(j)]
    for copy in ex_row:
        copy.wait_recv()
    dt_rows = jnp.zeros((CH, CH), F32)
    for slot in QS:
        for k in QS:
            i = img_at(slot, k) // CH
            tot = rsend[one(i), :]
            for p in ROW_PEERS:
                tot += rrecv[p - 1, one(img_at(slot ^ p, k) // CH), :]
            if slot == 0:
                loss_v += jnp.log(tot)
            fac = jnp.broadcast_to(INV / tot, (CH, CH)).T
            rs[at(i), :] = fac
            dt_rows += fac * ra[at(i), :]
    dt_v += scale * (jnp.sum(dt_rows, axis=0, keepdims=True) + jnp.sum(dt_cols, axis=0, keepdims=True))
    red[0] = jnp.concatenate([loss_v, dt_v, jnp.zeros((6, CH), F32)], axis=0)

    red_to = [to_x, to_zl, to_y, to_zh, to_c]
    ex_red = [remote(red.at[i], redr.at[i], sems(redm, i), to) for i, to in enumerate(red_to)]

    def red_step(i):
        ex_red[i].wait()
        red[i + 1] = red[i] + redr[i]
        if i + 1 < len(ex_red):
            ex_red[i + 1].start()

    ex_red[0].start()

    ri = lax.broadcasted_iota(jnp.int32, (CH, CH), 0)
    ci = lax.broadcasted_iota(jnp.int32, (CH, CH), 1)
    eye2 = jnp.where(ri == ci, 2.0 * INV, 0.0).astype(F32)

    def img_chunk(slot, k, buf, after):
        get_row(slot, k, buf).wait()
        after()
        fac = rs[rows_of(img_at(slot, k)), :]
        for j in range(NTX // CH):
            grow[:, at(j)] = (erow[buf, j] * (fac + bvec[:, at(j)])).astype(BF16)
        if slot == 0:
            j0 = pl.multiple_of(k * CH, CH)
            g = erow[buf, k] * (fac + bvec[:, pl.ds(j0, CH)])
            grow[:, pl.ds(j0, CH)] = (g - eye2).astype(BF16)
        return jnp.dot(grow[...], txts[...], preferred_element_type=F32)

    def txt_chunk(slot, k, buf, after):
        get_col(slot, k, buf).wait()
        after()
        b = bvec[:, pl.ds(pl.multiple_of(txt_at(slot, k), CH), CH)]
        gcol[...] = (ecol[buf] * (rs[...] + b)).astype(BF16)
        if slot == 0:
            own = rows_of(k * CH)
            g = ecol[buf, own, :] * (rs[own, :] + b)
            gcol[own, :] = (g - eye2).astype(BF16)
        return lax.dot_general(gcol[...], imgs[...], TN, preferred_element_type=F32)

    def half(h):
        return slice(CUTS[h], CUTS[h + 1])

    def c_x3(k, h):
        return remote(xb.at[3, k, half(h)], xb.at[1, k, half(h)], sems(x3, k, h), to_x)

    def c_x2(k):
        return remote(xb.at[2, k], xb.at[0, k], sems(x2, k), to_x)

    def c_zl(k, h):
        return remote(xb.at[1, k, half(h)], rzl.at[k, half(h)], sems(zls, k, h), to_zl)

    def c_core(slot, k):
        return remote(cb.at[slot - 4], rc.at[slot - 4, k], sems(core, slot - 4, k), to_c)

    def c_y3(k, h):
        return remote(rc.at[3, k, half(h)], ry.at[1, k, half(h)], sems(y3, k, h), to_y)

    def c_y2(k):
        return remote(rc.at[2, k], ry.at[0, k], sems(y2, k), to_y)

    def c_zh(k, h):
        return remote(rc.at[1, k, half(h)], rzh.at[k, half(h)], sems(zhs, k, h), to_zh)

    z_first = [remote(xb.at[3, 0, HEAD], rz.at[0], sems(zf, 0), to_zl), remote(rc.at[3, 0, HEAD], rz.at[1], sems(zf, 1), to_zh)]

    def when(cond, go):
        @pl.when(cond)
        def _():
            go()

    def fetch(cond, get):
        when(cond, lambda: get().start())

    def core_send(slot, k, buf, after):
        p = txt_chunk(slot, k, buf, after)
        when(k > 0, lambda: c_core(slot, k - 1).wait_send())
        cb[slot - 4] = p
        c_core(slot, k).start()

    def pass_zl(k, h):
        c_x3(k, h).wait_recv()
        xb[1, k, half(h)] += early[half(h)]
        c_zl(k, h).start()

    def pass_zh(k, h):
        c_y3(k, h).wait_recv()
        rc[1, k, half(h)] += ry[1, k, half(h)]
        c_zh(k, h).start()

    def step(t, _):
        k = t - 1
        km = t - (t + 3) // 4
        third, shift = t // 3, t // 4
        at0, at1, at3, at4, on = t == 0, t == 1, t == 3, t == 4, t > 0

        @pl.when(t < 4)
        def _():
            core_send(7, t, 0, lambda: get_col(3, t, 1).start())

            def row_after():
                fetch(at1, lambda: get_row(2, 0, 1))
                fetch(jnp.logical_not(at1), lambda: get_row(1, km, 1 - third))

            xb[3, t] = img_chunk(3, t, third, row_after)
            when(at0, z_first[0].start)
            when(on, lambda: c_x3(t, 0).start())
            for h in TWO:
                c_x3(t, h + 1).start()

            def col_after():
                fetch(at1, lambda: get_col(6, 0, 0))
                fetch(jnp.logical_not(at1), lambda: get_col(5, km, 0))

            p = txt_chunk(3, t, 1, col_after)
            c_core(7, t).wait_recv()
            rc[3, t] += p
            when(at0, z_first[1].start)
            when(on, lambda: c_y3(t, 0).start())
            for h in TWO:
                c_y3(t, h + 1).start()

        @pl.when(jnp.logical_not(at1))
        def _():
            core_send(5, km, 0, lambda: get_col(1, km, 1).start())

            def row_after():
                fetch(at0, lambda: get_row(3, 1, 0))
                fetch(on, lambda: get_row(2, k, (t + shift) % 2))

            early[...] = img_chunk(1, km, 1 - third, row_after)

            @pl.when(at0)
            def _():
                xb[1, 0, HEAD] = early[HEAD]
                c_zl(0, 0).start()

            def col_after():
                fetch(at0, lambda: get_col(7, 1, 0))
                fetch(on, lambda: get_col(6, k, 0))

            p = txt_chunk(1, km, 1, col_after)
            c_core(5, km).wait_recv()
            rc[1, km] += p
            when(at0, lambda: c_zh(0, 0).start())

            @pl.when(on)
            def _():
                pass_zl(km, 0)
                pass_zh(km, 0)

            pass_zl(km, 1)
            pass_zh(km, 1)

        @pl.when(on)
        def _():
            pass_zl(k, 2)
            pass_zh(k, 2)
            core_send(6, k, 0, lambda: get_col(2, k, 1).start())

            def row_after():
                fetch(t < 3, lambda: get_row(3, t + 1, (t + 1) // 3))
                fetch(at3, lambda: get_row(1, 3, 0))
                fetch(at4, lambda: get_row(0, 0, 0))

            xb[2, k] = img_chunk(2, k, (t + shift) % 2, row_after)

            @pl.when(at1)
            def _():
                z_first[0].wait_recv()
                xb[2, 0, HEAD] += rz[0]

            c_x2(k).start()

            def col_after():
                fetch(t < 3, lambda: get_col(7, t + 1, 0))
                fetch(at3, lambda: get_col(5, 3, 0))
                fetch(at4, lambda: get_col(4, 0, 0))

            p = txt_chunk(2, k, 1, col_after)
            c_core(6, k).wait_recv()
            rc[2, k] += p

            @pl.when(at1)
            def _():
                z_first[1].wait_recv()
                rc[2, 0, HEAD] += rz[1]

            c_y2(k).start()
            for i in QS:
                @pl.when(k == i)
                def _():
                    red_step(i)

        return 0

    def close(k, _):
        core_send(4, k, 0, lambda: get_col(0, k, 1).start())
        p = img_chunk(0, k, k % 2, lambda: fetch(k < 3, lambda: get_row(0, k + 1, (k + 1) % 2)))
        c_x2(k).wait_recv()
        xb[0, k] += p
        p = txt_chunk(0, k, 1, lambda: fetch(k < 3, lambda: get_col(4, k + 1, 0)))
        c_core(4, k).wait_recv()
        c_y2(k).wait_recv()
        rc[0, k] += p + ry[0, k]
        return 0

    lax.fori_loop(0, 5, step, 0)
    red_step(4)
    lax.fori_loop(0, 4, close, 0)
    loss_ref[0, 0] = jnp.sum(red[5, one(0), :]) * INV
    dt_ref[0, 0] = jnp.sum(red[5, one(1), :])

    wide = jnp.concatenate([scale] * (DIM // CH), axis=1)

    def out(n, k):
        src, dst = ((oimg, dimg_ref), (otxt, dtxt_ref))[n]
        return pltpu.make_async_copy(src.at[rows_of(k * CH), :], dst.at[rows_of(k * CH), :], s_out.at[n, k])

    def finish(k, _):
        for h in PARTS:
            c_zl(k, h).wait_recv()
        oimg[rows_of(k * CH), :] = (wide * (xb[0, k] + rzl[k])).astype(BF16)
        out(0, k).start()
        for h in PARTS:
            c_zh(k, h).wait_recv()
        otxt[rows_of(k * CH), :] = (wide * (rc[0, k] + rzh[k])).astype(BF16)
        out(1, k).start()
        return 0

    for copy in ex_col + ex_row + z_first:
        copy.wait_send()
    for k in QS:
        for copy in (g_zl, g_zh, g_x0, g_y0, g_x1, g_y1, c_x2, c_y2):
            copy(k).wait_send()
        for s in QS:
            g_c(s, k).wait_send()
        for h in PARTS:
            if k + h > 0:
                c_x3(k, h).wait_send()
                c_y3(k, h).wait_send()
        c_core(4 + k, 3).wait_send()
    lax.fori_loop(0, 4, finish, 0)

    for k in QS:
        for h in PARTS:
            for copy in (c_zl, c_zh):
                copy(k, h).wait_send()
        for n in TWO:
            out(n, k).wait()


def hand_over(img_ref, txt_ref, dimg_ref, dtxt_ref, buf, sem):
    parts = [(n, k) for k in TWO for n in TWO]

    def move(n, k, way):
        here = buf.at[n, pl.ds(k * PIECE, PIECE), :]
        there = ((img_ref, txt_ref), (dimg_ref, dtxt_ref))[way][n].at[pl.ds(k * PIECE, PIECE), :]
        src, dst = (here, there) if way else (there, here)
        return pltpu.make_async_copy(src, dst, sem.at[way, n, k])

    for n, k in parts:
        move(n, k, 0).start()
    for n, k in parts:
        move(n, k, 0).wait()
        move(n, k, 1).start()
    for n, k in parts:
        move(n, k, 1).wait()


def solution(mesh):
    spec = P(("row", "col"), None)
    smem = pl.BlockSpec(memory_space=pltpu.SMEM)
    hbm = pl.BlockSpec(memory_space=pl.ANY)
    v = pltpu.VMEM

    def dma(*shape):
        return pltpu.SemaphoreType.DMA(shape)

    def both(*shape):
        return dma(2, *shape)

    chunk = v((CH, DIM), F32)
    four, eight, sixteen = (v((*n, CH, DIM), F32) for n in ((4,), (2, 4), (4, 4)))
    image, text, own = (v((n, DIM), BF16) for n in (NI, NTX, ROWS))
    image_sums, text_sums = v((NI, CH), F32), v((8, NTX), F32)
    nr, nc = NI // CH, NTX // CH
    pieces = both(4, 3)
    scratch = [
        image, text, v((8, BLK // CH, PIECE, CH), F32),
        image_sums, image_sums, text_sums, text_sums, v((1, NTX), F32),
        v((2, nc, CH, CH), F32), v((2, NI, CH), F32), v((CH, NTX), BF16), v((NI, CH), BF16),
        sixteen, four, four, sixteen, eight, four,
        own, own, chunk, v((2, CUTS[1], DIM), F32),
        v((nr, CH), F32), v((3, nr, CH), F32), v((nc, CH), F32), v((7, nc, CH), F32), v((6, 8, CH), F32), v((5, 8, CH), F32),
        dma(2), dma(8), dma(2), dma(2), both(4),
        both(6, 4), both(4, 4), both(3), both(7), both(5),
        pieces, both(4), pieces, both(4, 4), pieces, both(4), pieces, both(2),
    ]
    shape = jax.ShapeDtypeStruct
    call = pl.pallas_call(
        kernel,
        out_shape=(shape((1, 1), F32), shape((ROWS, DIM), BF16), shape((ROWS, DIM), BF16), shape((1, 1), F32), shape((NTX // CH, NI, CH), F32)),
        in_specs=[smem, hbm, hbm],
        out_specs=(smem, hbm, hbm, smem, hbm),
        scratch_shapes=scratch,
        compiler_params=pltpu.CompilerParams(collective_id=0, has_side_effects=True, vmem_limit_bytes=67043328),
        name="clip",
    )
    final = pl.pallas_call(
        hand_over,
        out_shape=(shape((ROWS, DIM), BF16), shape((ROWS, DIM), BF16)),
        in_specs=[hbm, hbm],
        out_specs=(hbm, hbm),
        scratch_shapes=[v((2, ROWS, DIM), BF16), dma(2, 2, 2)],
        name="hand_over",
    )

    def local(img, txt, log_scale):
        loss, d_img, d_txt, dt, _ = call(log_scale.reshape(1), img, txt)
        d_img, d_txt = final(d_img, d_txt)
        return loss[0, 0], d_img, d_txt, dt[0, 0]

    return jax.shard_map(local, mesh=mesh, in_specs=(spec, spec, P()), out_specs=(P(), spec, spec, P()), check_vma=False)
```
